128 devices in a mesh: table: 32 (over z, x, core), sub: 4 (over y).
Axes of the slice: x: 4, y: 4, z: 4, core: 2. Of those that a mesh axis runs over, the one named last changes fastest.
Arguments:
- pooled: bfloat16 [96, 32, 4, 32, 128], P('table', None, 'sub'), may hold values from -6 to 6
- field_owner: int32 [48], replicated, may hold values from 0 to 31, as said below
- w_squeeze: float32 [16, 48], replicated, may hold values from -2.5 to 2.5
- w_excite: float32 [1536, 16], replicated, may hold values from -1.5 to 1.5
- w_bilinear: float32 [32, 32], replicated, may hold values from -1 to 1
- tower_weight: bfloat16 [36096, 1024], P(('table', 'sub')), may hold values from -0.1875 to 0.1875
- tower_cotangent: bfloat16 [1024, 16384], P(None, ('table', 'sub')), may hold values from -6 to 6
Outputs:
- row_grads: bfloat16 [96, 32, 4, 32, 128], P('table', None, 'sub')
- tower_weight_grad: float32 [36096, 1024], P(('table', 'sub'))
- squeeze_grad: float32 [16, 48], replicated
- excite_grad: float32 [1536, 16], replicated
- bilinear_grad: float32 [32, 32], replicated
The draws below stay inside these ranges and needn't reach their ends.
Inputs may be any that keep to these rules, and one draw needn't show every extreme that they name: `field_owner`: each table index holds at most 3 fields, and some index holds exactly 3.
All inputs are finite; a program needn't handle non-finite values.
Results may differ from the reference program's by a relative error of at most 0.0074.
Values may be sent and summed in bfloat16 or wider, within the bound.
No kernel may reach another device: no remote copies, remote signals or barrier semaphores. Data moves between devices by JAX's collectives and lax.ppermute only.
A program may use at most 192 MiB of HBM per device.

```python
import jax
import jax.numpy as jnp
from jax import lax

F = 48
E = 32
R = 16
H = 1024
B_DEV = 128
FSLOT = 3
SLOTS = 96
K = 36096
BATCH = 16384
N_TABLE = 32
N_SUB = 4


def draw_field_owner(key, part):
    first_key, order_key, shuffle_key = jax.random.split(jax.random.fold_in(key, 17), 3)
    capacity = N_TABLE * FSLOT
    favoured = jax.random.randint(first_key, (), 0, N_TABLE)
    positions = jnp.arange(capacity, dtype=jnp.int32)
    holders = positions // FSLOT
    scores = jax.random.permutation(order_key, capacity).astype(jnp.int32)
    scores = scores + jnp.where(holders == favoured, 0, capacity).astype(jnp.int32)
    ranked = jnp.argsort(scores, stable=True)
    chosen = ranked[:F] // FSLOT
    mixing = jax.random.permutation(shuffle_key, F)
    return chosen[mixing].astype(jnp.int32)


def levels(rng, shape, cuts, low, top_value):
    def one(dim, parts):
        steps = jax.random.uniform(jax.random.fold_in(jax.random.fold_in(rng, 6), dim), (parts,), jnp.float32, low / len(cuts), top_value / len(cuts))
        return jnp.repeat(jnp.exp(steps), shape[dim] // parts).reshape((-1,) + (1,) * (len(shape) - dim - 1))

    factor_of = one(*cuts[0])
    for cut in cuts[1:]:
        factor_of = factor_of * one(*cut)
    return factor_of


def bell_draw(key, extent, scale, limit, cuts=(), kind=jnp.bfloat16):
    gain = levels(key, extent, cuts, -0.22, 0.18) if cuts else 1.0
    drawn = jax.random.normal(key, extent, jnp.float32) * scale * gain
    return jnp.minimum(jnp.maximum(drawn, -limit), limit).astype(kind)


def setup_inputs(seed: int = 0) -> dict:
    streams_of = jax.random.split(jax.random.key(seed), 8)
    pooled = bell_draw(streams_of[0], (SLOTS, N_TABLE, N_SUB, E, B_DEV), 1.0, 6.0, ((0, 32), (2, 4)))
    field_owner = draw_field_owner(jax.random.fold_in(streams_of[7], 71), 0)
    w_squeeze = bell_draw(streams_of[2], (R, F), (F // 8) ** -0.5, 2.5, (), jnp.float32)
    w_excite = bell_draw(streams_of[3], (F * E, R), R ** -0.5, 1.5, (), jnp.float32)
    w_bilinear = bell_draw(streams_of[4], (E, E), E ** -0.5, 1.0, (), jnp.float32)
    tower_weight = bell_draw(streams_of[5], (K, H), H ** -0.5, 0.1875, ((0, 128),))
    tower_cotangent = bell_draw(streams_of[6], (H, BATCH), 1.0, 6.0, ((1, 128),))
    return dict(pooled=pooled, field_owner=field_owner, w_squeeze=w_squeeze, w_excite=w_excite, w_bilinear=w_bilinear, tower_weight=tower_weight, tower_cotangent=tower_cotangent)


def hadamard_table(width):
    index = jnp.arange(width, dtype=jnp.int32)
    both = index[:, None] & index[None, :]
    parity = jnp.zeros((width, width), jnp.int32)
    for bit_pos in range(width.bit_length()):
        parity = parity ^ both >> bit_pos & 1
    return (1 - 2 * parity).astype(jnp.float32)

def slot_table(field_owner, per_owner):
    count = field_owner.shape[0]
    order = jnp.arange(count, dtype=jnp.int32)
    same = field_owner[:, None] == field_owner[None, :]
    earlier = order[:, None] > order[None, :]
    position = lax.optimization_barrier(jnp.sum((same & earlier).astype(jnp.int32), axis=1))
    return (field_owner * per_owner + position).astype(jnp.int32)

def forward(fields, w_squeeze, w_excite, w_bilinear):
    count, width, samples = fields.shape
    high = lax.Precision.HIGHEST
    squeezed = lax.optimization_barrier(jnp.mean(fields, axis=1))
    activated = jax.nn.silu(jnp.dot(w_squeeze, squeezed, precision=high))
    excite = jnp.dot(w_excite, activated, precision=high).reshape(count, width, samples)
    weighted = fields * (1.0 + excite)
    mapped = jnp.einsum('ed,fen->fdn', w_bilinear, weighted, precision=high)
    pieces = [mapped[left][None] * weighted[left + 1:] for left in range(count - 1)]
    pairs = jnp.concatenate(pieces, axis=0)
    return pairs.reshape(-1, samples).astype(jnp.bfloat16)

def reference(pooled, field_owner, w_squeeze, w_excite, w_bilinear, tower_weight, tower_cotangent):
    groups = N_TABLE * N_SUB
    scale = 1.0 / E ** 0.5
    signs = hadamard_table(E)
    rotated = (jnp.einsum('ij,ktsjb->ktsib', signs, pooled.astype(jnp.float32)) * scale).astype(jnp.bfloat16)
    slot_index = slot_table(field_owner, FSLOT)
    chosen = jnp.take(rotated, slot_index, axis=0)
    chosen = jnp.transpose(chosen, (1, 2, 0, 3, 4)).reshape(groups, F, E, B_DEV)
    cotangent = jnp.transpose(tower_cotangent.reshape(H, groups, B_DEV), (1, 0, 2))

    def one_block(carry, inputs):
        weight_total, g_squeeze, g_excite, g_bilinear = carry
        block, grad_in = inputs
        fields = jnp.einsum('ij,fjn->fin', signs, block.astype(jnp.float32)) * scale
        pairs, back = jax.vjp(forward, fields, w_squeeze, w_excite, w_bilinear)
        weight_total = weight_total + jnp.dot(pairs, grad_in.T, preferred_element_type=jnp.float32)
        pair_grad = jnp.dot(tower_weight, grad_in, preferred_element_type=jnp.float32).astype(jnp.bfloat16)
        field_grad, d_squeeze, d_excite, d_bilinear = back(pair_grad)
        carry = (weight_total, g_squeeze + d_squeeze, g_excite + d_excite, g_bilinear + d_bilinear)
        return (carry, field_grad.astype(jnp.bfloat16))
    start = (jnp.zeros((K, H), jnp.float32), jnp.zeros((R, F), jnp.float32), jnp.zeros((F * E, R), jnp.float32), jnp.zeros((E, E), jnp.float32))
    totals, field_grads = lax.scan(one_block, start, (chosen, cotangent))
    onehot = (slot_index[None, :] == jnp.arange(SLOTS, dtype=jnp.int32)[:, None]).astype(jnp.float32)
    placed = jnp.einsum('sf,gfen->gsen', onehot, field_grads.astype(jnp.float32)).astype(jnp.bfloat16)
    placed = placed.reshape(N_TABLE, N_SUB, SLOTS, E, B_DEV)
    row_grads = jnp.transpose(placed, (2, 0, 1, 3, 4))
    inverse = 1.0 / BATCH
    return (row_grads, totals[0] * inverse, totals[1] * inverse, totals[2] * inverse, totals[3] * inverse)
```

```python
import jax
import jax.numpy as jnp
import numpy as np
from jax import lax
from jax.sharding import PartitionSpec as P

HIGH = lax.Precision.HIGHEST
BOTH = ("table", "sub")


def block_plan(tables):
    groups = int(round((2 * tables) ** 0.5))
    blocks = [(a, b) for a in range(groups) for b in range(a + 1, groups)]
    straight = len(blocks)
    blocks += [(a, a + 1) for a in range(0, groups, 2)]
    assert len(blocks) == tables
    return groups, straight, blocks


def color_edges(edges, left, right):
    degree_l = np.bincount([e[0] for e in edges], minlength=left)
    degree_r = np.bincount([e[1] for e in edges], minlength=right)
    colors = int(max(degree_l.max(), degree_r.max()))
    at_l = -np.ones((left, colors), int)
    at_r = -np.ones((right, colors), int)
    chosen = [-1] * len(edges)
    for k, (u, v) in enumerate(edges):
        a = int(np.where(at_l[u] < 0)[0][0])
        b = int(np.where(at_r[v] < 0)[0][0])
        if a != b:
            path, node, on_right, want = [], v, True, a
            while True:
                e = int((at_r if on_right else at_l)[node][want])
                if e < 0:
                    break
                path.append(e)
                node = edges[e][0] if on_right else edges[e][1]
                on_right = not on_right
                want = b if want == a else a
            for e in path:
                at_l[edges[e][0], chosen[e]] = -1
                at_r[edges[e][1], chosen[e]] = -1
            for e in path:
                chosen[e] = b if chosen[e] == a else a
                at_l[edges[e][0], chosen[e]] = e
                at_r[edges[e][1], chosen[e]] = e
        chosen[k] = a
        at_l[u, a] = k
        at_r[v, a] = k
    return colors, chosen


def row_plan(fields, tables, subs, width, rows):
    devices = tables * subs
    groups, straight, blocks = block_plan(tables)
    size = fields // groups
    share = size * size // subs
    pair_at = {}
    for i in range(fields):
        for j in range(i + 1, fields):
            pair_at[(i, j)] = len(pair_at)
    place = {}
    for r, (g, h) in enumerate(blocks):
        for a in range(size):
            for b in range(size):
                if r < straight:
                    pair = (g * size + a, h * size + b)
                elif a < b:
                    pair = (g * size + a, g * size + b)
                elif a > b:
                    pair = (h * size + b, h * size + a)
                else:
                    continue
                slot = a * size + b
                place[pair_at[pair]] = (r * subs + slot // share, slot % share)
    count = len(pair_at)
    assert len(place) == count and count * width == rows * devices
    first = [-(-rows * d // width) for d in range(devices + 1)]
    out_edges, out_info = [], []
    for g in range(count):
        d = width * g // rows
        out_edges.append((d, place[g][0]))
        out_info.append((g - first[d], place[g][1]))
    n_out, out_color = color_edges(out_edges, devices, devices)
    take = np.zeros((devices, n_out), np.int32)
    put = -np.ones((devices, share), np.int32)
    perms = [[] for _ in range(n_out)]
    used = np.zeros((devices, n_out), bool)
    for (u, v), (k, slot), c in zip(out_edges, out_info, out_color):
        perms[c].append((u, v))
        take[u, c] = width * first[u] - rows * u + width * k
        put[v, slot] = c
        used[v, c] = True
    for v in range(devices):
        for slot in range(share):
            if put[v, slot] < 0:
                put[v, slot] = int(np.where(~used[v])[0][0])
    back_edges, back_info = [], []
    low = [rows * d // width for d in range(devices)]
    span = 0
    for d in range(devices):
        for g in range(low[d], (rows * (d + 1) - 1) // width + 1):
            back_edges.append((place[g][0], d))
            back_info.append((place[g][1], g - low[d]))
            span = max(span, g - low[d] + 1)
    n_back, back_color = color_edges(back_edges, devices, devices)
    b_take = np.zeros((devices, n_back), np.int32)
    b_put = np.zeros((devices, span), np.int32)
    b_perms = [[] for _ in range(n_back)]
    for (u, v), (k, q), c in zip(back_edges, back_info, back_color):
        b_perms[c].append((u, v))
        b_take[u, c] = k
        b_put[v, q] = c
    b_off = np.array([rows * d - width * low[d] for d in range(devices)], np.int32)
    return dict(perms=perms, take=take, put=put, b_perms=b_perms, b_take=b_take, b_put=b_put, b_off=b_off)


def hadamard_table(width):
    index = jnp.arange(width, dtype=jnp.int32)
    both = index[:, None] & index[None, :]
    parity = jnp.zeros((width, width), jnp.int32)
    for bit_pos in range(width.bit_length()):
        parity = parity ^ both >> bit_pos & 1
    return (1 - 2 * parity).astype(jnp.bfloat16)


def slot_table(field_owner, per_owner):
    count = field_owner.shape[0]
    order = jnp.arange(count, dtype=jnp.int32)
    same = field_owner[:, None] == field_owner[None, :]
    earlier = order[:, None] > order[None, :]
    position = jnp.sum((same & earlier).astype(jnp.int32), axis=1)
    return field_owner * per_owner + position


def excited(fields, w_squeeze, w_excite):
    squeezed = jnp.mean(fields, axis=1)
    activated = jax.nn.silu(jnp.dot(w_squeeze, squeezed, precision=HIGH))
    excite = jnp.dot(w_excite, activated, precision=HIGH).reshape(fields.shape)
    return fields * (1.0 + excite)


def on_device(pooled, field_owner, w_squeeze, w_excite, w_bilinear, tower_weight, tower_cotangent):
    f32, bf16 = jnp.float32, jnp.bfloat16
    per_owner, _, _, width, samples = pooled.shape
    tables, subs = lax.axis_size("table"), lax.axis_size("sub")
    total_samples = tables * subs * samples
    count = field_owner.shape[0]
    rows, hidden = tower_weight.shape
    plan = row_plan(count, tables, subs, width, rows)
    groups, straight, blocks = block_plan(tables)
    size = count // groups
    scale = 1.0 / width**0.5
    signs = hadamard_table(width)
    me = lax.axis_index(BOTH)
    row_group = lax.axis_index("table")
    diag = row_group >= straight
    cols = tables * samples

    rotated = (
        jnp.einsum("ij,ktsjb->ktsib", signs, pooled, preferred_element_type=f32) * scale
    ).astype(bf16)
    received = lax.all_to_all(rotated, "table", split_axis=1, concat_axis=0, tiled=True)
    received = received.reshape(per_owner * tables, width, samples)
    slot_index = slot_table(field_owner, per_owner)
    selected = jnp.take(received, slot_index, axis=0)

    needed = np.array(blocks, np.int32).reshape(-1)
    by_group = selected.reshape(groups, size * width, samples)
    sent = jnp.concatenate([by_group[int(g)][None] for g in needed], axis=0)
    sent = sent.reshape(tables, 2 * size * width, samples)
    squeeze_rows = jnp.broadcast_to(selected[:, 0, :][None], (tables, count, samples))
    sent = jnp.concatenate([sent, squeeze_rows], axis=1)
    got = lax.all_to_all(sent, "table", split_axis=0, concat_axis=0, tiled=True)
    got = jnp.moveaxis(got, 0, 1).reshape(2 * size * width + count, cols)

    nearby = lax.ppermute(
        tower_weight[:width], BOTH, [(d + 1, d) for d in range(tables * subs - 1)]
    )
    extended = jnp.concatenate([tower_weight, nearby], axis=0)
    take = jnp.asarray(plan["take"])[me]
    arrived = []
    for c, perm in enumerate(plan["perms"]):
        piece = lax.dynamic_slice(extended, (take[c], 0), (width, hidden))
        arrived.append(lax.ppermute(piece, BOTH, perm))
    mine = jnp.take(jnp.stack(arrived), jnp.asarray(plan["put"])[me], axis=0)
    mine = mine.reshape(-1, hidden)
    weights = lax.all_to_all(
        jnp.broadcast_to(mine[None], (subs, *mine.shape)), "sub", 0, 0, tiled=True
    ).reshape(-1, hidden)

    cotangent = lax.all_gather(tower_cotangent, "table", axis=1, tiled=True)
    pair_grad = jnp.dot(weights, cotangent, preferred_element_type=f32).astype(bf16)
    pair_grad = pair_grad.reshape(size, size, width, cols)

    chosen = got[: 2 * size * width].reshape(2 * size, width, cols)
    fields = jnp.einsum("ij,fjn->fin", signs, chosen, preferred_element_type=f32) * scale
    squeezed = got[2 * size * width :].astype(f32) * scale
    activated = jax.nn.silu(jnp.dot(w_squeeze, squeezed, precision=HIGH))
    mine_groups = jnp.asarray(np.array(blocks, np.int32))[row_group]
    w_here = jnp.take(w_excite.reshape(groups, size * width, -1), mine_groups, axis=0)
    w_here = w_here.reshape(2 * size * width, -1)
    excite = jnp.dot(w_here, activated, precision=HIGH).reshape(fields.shape)
    weighted = fields * (1.0 + excite)
    mapped = jnp.einsum("ed,fen->fdn", w_bilinear, weighted, precision=HIGH)
    m1, m2, w1, w2 = mapped[:size], mapped[size:], weighted[:size], weighted[size:]
    x_up, x_lo = m1, jnp.where(diag, w2, m1)
    y_up, y_lo = jnp.where(diag, w1, w2), jnp.where(diag, m2, w2)

    pg = pair_grad.astype(f32)
    zero = jnp.zeros((width, cols), f32)
    dx_up = jnp.stack([sum((pg[a, b] * y_up[b] for b in range(a + 1, size)), zero) for a in range(size)])
    dx_lo = jnp.stack([sum((pg[a, b] * y_lo[b] for b in range(a + 1)), zero) for a in range(size)])
    dy_up = jnp.stack([sum((pg[a, b] * x_up[a] for a in range(b)), zero) for b in range(size)])
    dy_lo = jnp.stack([sum((pg[a, b] * x_lo[a] for a in range(b, size)), zero) for b in range(size)])
    dm = jnp.concatenate([dx_up + jnp.where(diag, 0.0, dx_lo), jnp.where(diag, dy_lo, 0.0)], axis=0)
    dw = jnp.concatenate(
        [jnp.where(diag, dy_up, 0.0), jnp.where(diag, dx_lo, dy_up + dy_lo)], axis=0
    )
    d_bilinear = jnp.einsum("fen,fdn->ed", weighted, dm, precision=HIGH)
    part = dw + jnp.einsum("ed,fdn->fen", w_bilinear, dm, precision=HIGH)
    part = part.astype(bf16).reshape(2 * size * width, tables, samples)
    part = jnp.moveaxis(part, 1, 0)
    parts = lax.all_to_all(part, "table", split_axis=0, concat_axis=0, tiled=True)

    pairs = jnp.stack(
        [
            jnp.concatenate(
                [x_lo[a][None] * y_lo[: a + 1], x_up[a][None] * y_up[a + 1 :]], axis=0
            )
            for a in range(size)
        ]
    )
    pairs = pairs.astype(bf16).reshape(size * size * width, cols)
    total = lax.dot_general(
        pairs, cotangent, (((1,), (1,)), ((), ())), preferred_element_type=f32
    )
    total = total.astype(bf16).reshape(subs, -1, hidden)
    total = lax.all_to_all(total, "sub", 0, 0, tiled=True)
    total = jnp.sum(total.astype(f32), axis=0) * (1.0 / total_samples)
    total = total.astype(bf16).reshape(-1, width, hidden)
    b_take = jnp.asarray(plan["b_take"])[me]
    arrived = []
    for c, perm in enumerate(plan["b_perms"]):
        piece = lax.dynamic_slice(total, (b_take[c], 0, 0), (1, width, hidden))[0]
        arrived.append(lax.ppermute(piece, BOTH, perm))
    rows_back = jnp.take(jnp.stack(arrived), jnp.asarray(plan["b_put"])[me], axis=0)
    rows_back = rows_back.reshape(-1, hidden)
    weight_grad = lax.dynamic_slice(
        rows_back, (jnp.asarray(plan["b_off"])[me], 0), (rows, hidden)
    ).astype(f32)

    collect = np.zeros((groups, 2 * tables), np.float32)
    for k, g in enumerate(needed):
        collect[g, k] = 1.0
    d_weighted = jnp.einsum(
        "gk,ken->gen",
        jnp.asarray(collect, bf16),
        parts.reshape(2 * tables, size * width, samples),
        preferred_element_type=f32,
    ).reshape(count, width, samples)
    own = jnp.einsum("ij,fjn->fin", signs, selected, preferred_element_type=f32) * scale
    _, back = jax.vjp(excited, own, w_squeeze, w_excite)
    field_grad, d_squeeze, d_excite = back(d_weighted)
    g_squeeze, g_excite, g_bilinear = lax.psum((d_squeeze, d_excite, d_bilinear), BOTH)
    slot_count = per_owner * tables
    onehot = (slot_index[None, :] == jnp.arange(slot_count, dtype=jnp.int32)[:, None]).astype(bf16)
    placed = jnp.einsum(
        "sf,fen->sen", onehot, field_grad.astype(bf16), preferred_element_type=f32
    ).astype(bf16)
    placed = placed.reshape(slot_count, 1, 1, width, samples)
    row_grads = lax.all_to_all(placed, "table", split_axis=0, concat_axis=1, tiled=True)
    inverse = 1.0 / total_samples
    return (row_grads, weight_grad, g_squeeze * inverse, g_excite * inverse, g_bilinear * inverse)


def solution(mesh):
    return jax.shard_map(
        on_device,
        mesh=mesh,
        in_specs=(
            P("table", None, "sub", None, None),
            P(),
            P(),
            P(),
            P(),
            P(BOTH, None),
            P(None, BOTH),
        ),
        out_specs=(P("table", None, "sub", None, None), P(BOTH, None), P(), P(), P()),
        check_vma=False,
    )
```

```python
import functools

import jax
import jax.numpy as jnp
import numpy as np
from jax import lax
from jax.experimental import pallas as pl
from jax.experimental.pallas import tpu as pltpu
from jax.sharding import PartitionSpec as P

HIGH = lax.Precision.HIGHEST
BOTH = ("table", "sub")
PLANES = 4
LIMIT = 13

WORKER = (
    4, 3, 2, 5, 0, 2, 4, 3, 7, 3, 0, 4, 6, 2, 2, 6, 6, 3, 4, 0, 3, 7, 1, 1, 5, 7, 6, 0, 5, 6, 7, 1, 2, 1, 5, 5, 1, 4, 3, 2, 2, 4, 7, 7, 0, 1, 5,
    5, 0, 6, 1, 6, 4, 3, 7, 3, 0, 4, 6, 2, 2, 1, 6, 3, 4, 0, 3, 0, 2, 1, 6, 7, 6, 0, 5, 6, 7, 1, 2, 1, 5, 5, 1, 4, 3, 2, 2, 4, 7, 7, 0, 1, 5, 1,
    5, 4, 3, 4, 3, 7, 3, 0, 4, 6, 2, 2, 6, 6, 3, 4, 0, 3, 7, 2, 1, 6, 7, 6, 0, 5, 6, 7, 1, 2, 1, 5, 5, 1, 4, 3, 2, 2, 4, 5, 7, 0, 1, 5, 7, 3, 4,
    4, 3, 7, 3, 0, 4, 6, 2, 2, 6, 6, 3, 4, 0, 3, 0, 1, 1, 5, 7, 6, 0, 5, 6, 7, 1, 2, 1, 5, 5, 1, 4, 3, 2, 2, 4, 5, 7, 0, 5, 5, 1, 7, 4, 3, 7, 3,
    0, 4, 6, 2, 2, 6, 6, 3, 4, 0, 3, 0, 2, 1, 5, 7, 6, 0, 5, 6, 7, 1, 2, 1, 5, 5, 1, 4, 3, 2, 2, 4, 5, 7, 0, 5, 5, 0, 4, 3, 7, 3, 0, 4, 6, 2, 2,
    6, 6, 3, 4, 0, 3, 7, 2, 1, 6, 7, 6, 0, 5, 6, 7, 1, 2, 1, 5, 5, 1, 4, 3, 2, 2, 4, 7, 7, 0, 5, 5, 4, 3, 7, 3, 0, 4, 6, 2, 2, 6, 6, 3, 4, 0, 3,
    1, 5, 7, 6, 6, 4, 0, 1, 5, 2, 1, 4, 7, 0, 6, 0, 6, 3, 4, 7, 1, 7, 3, 0, 3, 5, 6, 0, 2, 3, 2, 4, 3, 2, 4, 1, 5, 3, 2, 2, 1, 5, 7, 6, 6, 4, 0,
    1, 5, 2, 1, 4, 7, 0, 6, 0, 6, 3, 4, 7, 1, 7, 3, 0, 3, 5, 7, 4, 3, 6, 5, 3, 2, 4, 1, 5, 3, 2, 2, 1, 5, 7, 6, 6, 4, 2, 1, 5, 2, 1, 4, 7, 0, 6,
    0, 6, 3, 4, 7, 1, 7, 6, 0, 3, 5, 7, 0, 3, 5, 3, 2, 4, 1, 5, 3, 2, 2, 1, 5, 7, 0, 6, 4, 2, 1, 5, 2, 1, 4, 7, 0, 6, 0, 6, 3, 4, 7, 1, 7, 3, 0,
    3, 5, 3, 7, 5, 3, 2, 4, 1, 5, 3, 2, 2, 1, 5, 7, 0, 6, 4, 2, 1, 5, 2, 1, 4, 7, 0, 6, 0, 6, 3, 4, 7, 1, 7, 6, 0, 3, 5, 5, 4, 3, 2, 4, 1, 5, 3,
    2, 2, 1, 5, 7, 0, 6, 4, 0, 1, 5, 2, 1, 4, 7, 0, 6, 0, 6, 3, 4, 7, 1, 7, 3, 0, 3, 5, 2, 3, 2, 4, 1, 5, 3, 2, 2, 1, 5, 7, 0, 6, 4, 0, 1, 5, 2,
    1, 4, 7, 0, 6, 0, 6, 3, 4, 7, 1, 7, 6, 0, 3, 5, 3, 2, 4, 1, 5, 3, 2, 2, 1, 5, 7, 0, 6, 4, 2, 1, 5, 2, 1, 4, 7, 0, 6, 0, 6, 3, 4, 7, 1, 7, 6,
    7, 7, 7, 3, 5, 4, 0, 6, 0, 5, 2, 1, 5, 4, 2, 6, 1, 3, 0, 0, 3, 2, 4, 1, 5, 4, 5, 0, 3, 1, 2, 6, 6, 7, 7, 7, 4, 7, 4, 2, 3, 2, 0, 0, 5, 4, 2,
    6, 1, 3, 0, 0, 3, 2, 4, 1, 5, 4, 5, 0, 3, 1, 2, 6, 6, 7, 7, 7, 6, 1, 1, 2, 1, 3, 6, 5, 4, 2, 6, 1, 3, 0, 0, 3, 2, 4, 1, 5, 4, 5, 0, 3, 1, 2,
    6, 6, 7, 7, 7, 4, 3, 0, 6, 5, 2, 5, 4, 2, 6, 1, 3, 0, 0, 3, 2, 4, 1, 5, 4, 5, 0, 3, 1, 2, 6, 6, 7, 7, 7, 7, 0, 7, 4, 6, 5, 4, 2, 6, 1, 3, 0,
    0, 3, 2, 4, 1, 5, 4, 5, 0, 3, 1, 2, 6, 6, 7, 7, 7, 2, 6, 7, 6, 5, 4, 2, 6, 1, 3, 0, 0, 3, 2, 4, 1, 5, 4, 5, 0, 3, 1, 2, 6, 6, 7, 7, 7, 3, 0,
    1, 5, 4, 2, 6, 1, 3, 0, 0, 3, 2, 4, 1, 5, 4, 5, 0, 3, 1, 2, 6, 6, 7, 7, 7, 5, 3, 5, 4, 2, 6, 1, 3, 0, 0, 3, 2, 4, 1, 5, 4, 5, 0, 3, 1, 2, 6,
    6, 7, 7, 7, 6, 5, 4, 2, 6, 1, 3, 0, 0, 3, 2, 4, 1, 5, 4, 5, 0, 3, 1, 2, 6, 6, 7, 7, 7, 5, 4, 2, 6, 1, 3, 0, 0, 3, 2, 4, 1, 5, 4, 5, 0, 3, 1,
    6, 6, 6, 1, 1, 1, 3, 5, 7, 5, 7, 0, 7, 0, 5, 0, 2, 3, 0, 5, 2, 0, 2, 5, 7, 3, 2, 7, 3, 3, 4, 2, 4, 1, 1, 4, 1, 3, 2, 3, 4, 2, 2, 4, 2, 4, 4,
    3, 2, 1, 1, 0, 6, 7, 5, 0, 0, 7, 3, 6, 6, 7, 5, 0, 5, 6, 7, 5, 6, 3, 7, 3, 6, 4, 6, 7, 3, 7, 0, 6, 7, 4, 3, 3, 0, 0, 4, 6, 4, 4, 7, 3, 1, 1,
    5, 2, 1, 2, 6, 1, 5, 2, 2, 1, 2, 5, 5, 6, 2, 6, 5, 1, 7, 4, 1, 4, 2, 7, 4, 2, 7, 1, 2, 4, 2, 7, 4, 7, 1, 5, 3, 0, 3, 6, 3, 0, 3, 0, 1, 6, 5,
    6, 6, 1, 6, 6, 5, 7, 4, 4, 1, 7, 5, 0, 1, 0, 7, 5, 7, 4, 7, 1, 5, 0, 2, 3, 5, 2, 3, 4, 0, 4, 2, 0, 3, 2, 3, 0, 1, 7, 5, 5, 7, 5, 0, 5, 5, 7,
    1, 1, 1, 2, 3, 4, 3, 0, 4, 0, 4, 4, 0, 3, 2, 3, 6, 4, 2, 2, 1, 6, 6, 6, 4, 2, 1, 1, 7, 3, 3, 1, 6, 6, 6, 3, 1, 6, 1, 5, 7, 0, 0, 4, 4, 4, 4,
    7, 5, 3, 5, 2, 5, 2, 3, 2, 2, 5, 0, 0, 7, 2, 3, 2, 2, 3, 0, 4, 5, 0, 1, 1, 5, 6, 6, 0, 2, 2, 6, 5, 6, 4, 7, 5, 7, 4, 7, 5, 3, 7, 3, 1, 1, 6,
)


@functools.lru_cache(maxsize=None)
def make_plan(count, tables, subs, width, rows):
    plane = tables // PLANES
    held = rows * subs
    unit = 8
    assert width % unit == 0 and held % unit == 0
    pairs = [(i, j) for i in range(count) for j in range(i + 1, count)]
    assert len(pairs) == len(WORKER) and len(pairs) * width == held * tables
    per_plane = len(pairs) // PLANES
    worker = [plane * (g // per_plane) + WORKER[g] for g in range(len(pairs))]
    fields = [set() for _ in range(tables)]
    for g, r in enumerate(worker):
        fields[r] |= set(pairs[g])
    fields = [sorted(s) for s in fields]
    assert max(len(s) for s in fields) <= LIMIT
    table = np.zeros((tables, LIMIT), np.int32)
    live = np.zeros((tables, LIMIT), bool)
    for r, s in enumerate(fields):
        table[r, : len(s)] = s
        live[r, : len(s)] = True
    touched = [[[] for _ in range(plane)] for _ in range(tables)]
    for t in range(tables):
        for g in range(held * t // width, (held * (t + 1) - 1) // width + 1):
            assert worker[g] // plane == t // plane
            touched[t][worker[g] % plane].append(g)
    depth = max(len(x) for y in touched for x in y)
    units = held // unit
    per = width // unit
    pick = np.full((tables, plane, depth, per), units, np.int32)
    back = np.zeros((tables, units), np.int32)
    left = np.zeros((tables, plane * depth), np.int32)
    right = np.zeros((tables, plane * depth), np.int32)
    for t in range(tables):
        for w in range(plane):
            for c, g in enumerate(touched[t][w]):
                r = t // plane * plane + w
                slot = (t % plane) * depth + c
                left[r, slot] = fields[r].index(pairs[g][0])
                right[r, slot] = fields[r].index(pairs[g][1])
                for q in range(per):
                    u = (width * g - held * t) // unit + q
                    if 0 <= u < units:
                        pick[t, w, c, q] = u
                        back[t, u] = (w * depth + c) * per + q
    return dict(
        table=table, live=live, depth=depth, pick=pick.reshape(tables, -1), back=back,
        left=left, right=right, plane=plane, unit=unit, units=units,
    )


def hadamard_np(width):
    index = np.arange(width)
    both = index[:, None] & index[None, :]
    parity = np.zeros((width, width), int)
    for bit_pos in range(width.bit_length()):
        parity = parity ^ (both >> bit_pos & 1)
    return (1 - 2 * parity).astype(np.float32)


def slot_table(field_owner, per_owner):
    count = field_owner.shape[0]
    order = jnp.arange(count, dtype=jnp.int32)
    same = field_owner[:, None] == field_owner[None, :]
    earlier = order[:, None] > order[None, :]
    position = jnp.sum((same & earlier).astype(jnp.int32), axis=1)
    return field_owner * per_owner + position


def excited(fields, squeezed, w_squeeze, w_excite):
    activated = jax.nn.silu(jnp.dot(w_squeeze, squeezed, precision=HIGH))
    excite = jnp.dot(w_excite, activated, precision=HIGH).reshape(fields.shape)
    return fields * (1.0 + excite)


def partner_order(values, axis, group):
    own = lax.axis_index(axis) % group
    stacked = jnp.stack(values)
    return jnp.take(stacked, own ^ jnp.arange(group, dtype=jnp.int32), axis=0)


def swap(value, axis, size, k):
    return lax.ppermute(value, axis, [(a, a ^ k) for a in range(size)])


def trade(blocks, axis, size, group):
    own = lax.axis_index(axis) % group
    sent = [lax.dynamic_index_in_dim(blocks, own ^ k, 0, False) for k in range(group)]
    got = [sent[0]] + [swap(sent[k], axis, size, k) for k in range(1, group)]
    return partner_order(got, axis, group)


def spread(value, axis, size):
    got = [value] + [swap(value, axis, size, k) for k in range(1, size)]
    return partner_order(got, axis, size)


def halves(x):
    high = x.astype(jnp.bfloat16)
    return high, (x - high.astype(jnp.float32)).astype(jnp.bfloat16)


def pack_rows(received, squeezed, index, tables):
    slots, width, samples = received.shape
    count = squeezed.shape[0]
    total = LIMIT * width + count
    turn = 8

    def body(index_ref, received_ref, squeezed_ref, out_ref):
        first = pl.program_id(0) * (turn * LIMIT)
        for r in range(turn):
            for k in range(LIMIT):
                out_ref[r, k * width : (k + 1) * width, :] = received_ref[
                    index_ref[first + r * LIMIT + k]
                ]
            out_ref[r, LIMIT * width :, :] = squeezed_ref[...]

    return pl.pallas_call(
        body,
        out_shape=jax.ShapeDtypeStruct((tables, total, samples), received.dtype),
        grid_spec=pltpu.PrefetchScalarGridSpec(
            num_scalar_prefetch=1,
            grid=(tables // turn,),
            in_specs=[
                pl.BlockSpec((slots, width, samples), lambda i, *_: (0, 0, 0)),
                pl.BlockSpec((count, samples), lambda i, *_: (0, 0)),
            ],
            out_specs=pl.BlockSpec((turn, total, samples), lambda i, *_: (i, 0, 0)),
        ),
        name="pack_rows",
    )(index, received, squeezed)


def pair_step(got, pair_grad, left, right, signs, w_map, w_back, w_ex, w_ext, w_sq, extra, width):
    tables, tall, samples = got.shape
    slots = left.shape[0]
    units = w_sq.shape[0]
    count = tall - LIMIT * width
    span = LIMIT * width
    group = 4
    cols = group * samples
    scale = 1.0 / width**0.5
    f32, bf16 = jnp.float32, jnp.bfloat16

    def dot(a, b):
        return jnp.dot(a, b, preferred_element_type=f32)

    def dot_nt(a, b):
        return lax.dot_general(a, b, (((1,), (1,)), ((), ())), preferred_element_type=f32)

    def body(left_ref, right_ref, got_ref, pg_ref, hd_ref, mh_ref, ml_ref, bh_ref, bl_ref,
             wex_ref, wext_ref, wsq_ref, pairs_ref, part_ref, dbil_ref, dex_ref, dsq_ref,
             wt, mp, dm, dw):
        rows = jnp.concatenate([got_ref[o] for o in range(group)], axis=1)
        sq = rows[span:]
        fields = dot(hd_ref[...], rows[:span]) * scale
        pre = dot(wsq_ref[...], jnp.concatenate([sq, sq, sq], axis=0)) * scale
        gate = 1.0 / (1.0 + jnp.exp(-pre))
        act = pre * gate
        ah, al = halves(act)
        excite = dot(wex_ref[...], jnp.concatenate([ah, ah, al], axis=0))
        weighted = fields * (1.0 + excite)
        wh, wl = halves(weighted)
        mapped = dot(mh_ref[...], wh) + dot(mh_ref[...], wl) + dot(ml_ref[...], wh)
        wt[...] = weighted.reshape(LIMIT, width, cols)
        mp[...] = mapped.reshape(LIMIT, width, cols)
        dm[...] = jnp.zeros_like(dm)
        dw[...] = jnp.zeros_like(dw)

        def one(p, carry):
            i = left_ref[p]
            j = right_ref[p]
            off = pl.multiple_of(p * width, width)
            x = mp[i]
            y = wt[j]
            pairs_ref[pl.ds(off, width), :] = (x * y).astype(bf16)
            g = pg_ref[pl.ds(off, width), :].astype(f32)
            dm[i] += g * y
            dw[j] += g * x
            return carry

        lax.fori_loop(0, slots, one, 0)
        dmv = dm[...].reshape(span, cols)
        dh, dl = halves(dmv)
        part = dw[...].reshape(span, cols) + (
            dot(bh_ref[...], dh) + dot(bh_ref[...], dl) + dot(bl_ref[...], dh)
        )
        sent = part.astype(bf16)
        for o in range(group):
            part_ref[o, :span] = sent[:, o * samples : (o + 1) * samples]
            part_ref[o, span:] = jnp.zeros((extra, samples), bf16)
        d_excite = part * fields
        eh, el = halves(d_excite)
        d_act = dot(wext_ref[...], jnp.concatenate([eh, el, eh], axis=0))
        d_pre = d_act * gate * (1.0 + pre * (1.0 - gate))
        ph, pl_ = halves(d_pre)

        @pl.when(pl.program_id(0) == 0)
        def _():
            dbil_ref[...] = jnp.zeros_like(dbil_ref)
            dex_ref[...] = jnp.zeros_like(dex_ref)
            dsq_ref[...] = jnp.zeros_like(dsq_ref)

        dbil_ref[...] += dot_nt(wh, dh)
        dex_ref[...] += dot_nt(jnp.concatenate([ah, al], axis=0), eh)
        dsq_ref[...] += dot_nt(jnp.concatenate([ph, pl_], axis=0), sq)

    def whole(a):
        return pl.BlockSpec(a.shape, lambda i, *_: (0, 0))

    mats = (signs, *w_map, *w_back, w_ex, w_ext, w_sq)
    return pl.pallas_call(
        body,
        out_shape=(
            jax.ShapeDtypeStruct((slots * width, tables * samples), bf16),
            jax.ShapeDtypeStruct((tables, span + extra, samples), bf16),
            jax.ShapeDtypeStruct((span, span), f32),
            jax.ShapeDtypeStruct((2 * units, span), f32),
            jax.ShapeDtypeStruct((2 * units, count), f32),
        ),
        grid_spec=pltpu.PrefetchScalarGridSpec(
            num_scalar_prefetch=2,
            grid=(tables // group,),
            in_specs=[
                pl.BlockSpec((group, got.shape[1], samples), lambda i, *_: (i, 0, 0)),
                pl.BlockSpec((slots * width, cols), lambda i, *_: (0, i)),
                *[whole(m) for m in mats],
            ],
            out_specs=[
                pl.BlockSpec((slots * width, cols), lambda i, *_: (0, i)),
                pl.BlockSpec((group, span + extra, samples), lambda i, *_: (i, 0, 0)),
                pl.BlockSpec((span, span), lambda i, *_: (0, 0)),
                pl.BlockSpec((2 * units, span), lambda i, *_: (0, 0)),
                pl.BlockSpec((2 * units, count), lambda i, *_: (0, 0)),
            ],
            scratch_shapes=[pltpu.VMEM((LIMIT, width, cols), f32) for _ in range(4)],
        ),
        compiler_params=pltpu.CompilerParams(vmem_limit_bytes=40 * 1024 * 1024),
        name="pair_step",
    )(left, right, got, pair_grad, *mats)


def on_device(pooled, field_owner, w_squeeze, w_excite, w_bilinear, tower_weight, tower_cotangent):
    f32, bf16 = jnp.float32, jnp.bfloat16
    per_owner, _, _, width, samples = pooled.shape
    tables, subs = lax.axis_size("table"), lax.axis_size("sub")
    total_samples = tables * subs * samples
    count = field_owner.shape[0]
    rows, hidden = tower_weight.shape
    plan = make_plan(count, tables, subs, width, rows)
    plane, depth, unit, units = plan["plane"], plan["depth"], plan["unit"], plan["units"]
    quarter = hidden // subs
    scale = 1.0 / width**0.5
    signs_np = hadamard_np(width)
    signs = jnp.asarray(signs_np, bf16)
    here = lax.axis_index("table")

    rotated = (
        jnp.einsum("ij,ktsjb->ktsib", signs, pooled, preferred_element_type=f32) * scale
    ).astype(bf16)
    received = lax.all_to_all(rotated, "table", split_axis=1, concat_axis=0, tiled=True)
    received = received.reshape(per_owner * tables, width, samples)
    slot_index = slot_table(field_owner, per_owner)
    selected = jnp.take(received, slot_index, axis=0)
    squeeze_rows = selected[:, 0, :]
    wanted = slot_index[jnp.asarray(plan["table"].reshape(-1))]
    sent = pack_rows(received, squeeze_rows, wanted, tables)
    got = lax.all_to_all(sent, "table", split_axis=0, concat_axis=0, tiled=True)

    cut = jnp.moveaxis(tower_weight.reshape(rows, subs, quarter), 1, 0)
    cut = trade(cut, "sub", subs, subs).reshape(units, unit, quarter)
    cut = jnp.concatenate([cut, jnp.zeros((1, unit, quarter), bf16)], axis=0)
    cut = jnp.take(cut, jnp.asarray(plan["pick"])[here], axis=0)
    cut = cut.reshape(plane, depth * width, quarter)
    cut = trade(cut, "table", tables, plane)
    cut = cut.reshape(plane * depth * width, quarter)
    weights = spread(cut, "sub", subs)
    weights = jnp.moveaxis(weights, 0, 1).reshape(-1, hidden)

    cotangent = lax.all_gather(tower_cotangent, "table", axis=1, tiled=True)
    pair_grad = jnp.dot(weights, cotangent, preferred_element_type=f32).astype(bf16)

    eye = jnp.eye(LIMIT, dtype=f32)
    w_here = jnp.take(
        w_excite.reshape(count, width, -1), jnp.asarray(plan["table"])[here], axis=0
    ).reshape(LIMIT * width, -1)
    xh, xl = halves(w_here)
    s1, rest = halves(w_squeeze)
    s2 = rest
    s3 = (w_squeeze - s1.astype(f32) - s2.astype(f32)).astype(bf16)
    hidden_units = w_squeeze.shape[0]
    small_size = w_squeeze.size + w_excite.size + w_bilinear.size
    each = -(-small_size // (tables * samples)) * samples
    extra = -(-2 * each // samples // 16) * 16
    pairs, part, d_bilinear, d_excite, d_squeeze = pair_step(
        got,
        pair_grad,
        jnp.asarray(plan["left"])[here],
        jnp.asarray(plan["right"])[here],
        jnp.asarray(np.kron(np.eye(LIMIT), signs_np), bf16),
        halves(jnp.kron(eye, w_bilinear.T)),
        halves(jnp.kron(eye, w_bilinear)),
        jnp.concatenate([xh, xl, xh], axis=1),
        jnp.concatenate([xh, xh, xl], axis=0).T,
        jnp.concatenate([s1, s2, s3], axis=1),
        extra,
        width,
    )
    d_bilinear = jnp.sum(
        jnp.stack(
            [d_bilinear[k : k + width, k : k + width] for k in range(0, LIMIT * width, width)]
        ),
        axis=0,
    )
    d_excite = d_excite[:hidden_units] + d_excite[hidden_units:]
    d_squeeze = d_squeeze[:hidden_units] * scale + d_squeeze[hidden_units:] * scale
    lift = (
        jnp.arange(count, dtype=jnp.int32)[:, None] == jnp.asarray(plan["table"])[here][None, :]
    ) & jnp.asarray(plan["live"])[here][None, :]
    d_excite = d_excite.reshape(hidden_units, LIMIT, width).transpose(1, 2, 0)
    d_excite = jnp.dot(
        lift.astype(f32), d_excite.reshape(LIMIT, width * hidden_units), precision=HIGH
    )
    small = jnp.concatenate([d_excite.reshape(-1), d_squeeze.reshape(-1), d_bilinear.reshape(-1)])
    small = jnp.concatenate([small, jnp.zeros((tables * each - small_size,), f32)])
    small = jnp.concatenate(
        [h.reshape(tables, each // samples, samples) for h in halves(small)], axis=1
    )
    part = lax.dynamic_update_slice(part, small, (0, LIMIT * width, 0))
    parts = lax.all_to_all(part, "table", split_axis=0, concat_axis=0, tiled=True)
    total = lax.dot_general(
        pairs, cotangent, (((1,), (1,)), ((), ())), preferred_element_type=f32
    )
    total = jnp.moveaxis(total.astype(bf16).reshape(-1, subs, quarter), 1, 0)
    total = trade(total, "sub", subs, subs)
    total = (jnp.sum(total.astype(f32), axis=0) * (1.0 / total_samples)).astype(bf16)
    total = total.reshape(plane, depth * width, quarter)
    total = trade(total, "table", tables, plane)
    total = total.reshape(-1, unit, quarter)
    total = jnp.take(total, jnp.asarray(plan["back"])[here], axis=0)
    total = total.reshape(subs, rows, quarter)
    total = trade(total, "sub", subs, subs)
    weight_grad = jnp.moveaxis(total, 0, 1).reshape(rows, hidden).astype(f32)

    gather = np.zeros((count, tables * LIMIT), np.float32)
    for r in range(tables):
        for k in range(LIMIT):
            if plan["live"][r, k]:
                gather[plan["table"][r, k], r * LIMIT + k] = 1.0
    d_weighted = jnp.einsum(
        "gk,ken->gen",
        jnp.asarray(gather, bf16),
        parts[:, : LIMIT * width].reshape(tables * LIMIT, width, samples),
        preferred_element_type=f32,
    )
    own = jnp.einsum("ij,fjn->fin", signs, selected, preferred_element_type=f32) * scale
    squeezed = squeeze_rows.astype(f32) * scale
    _, back = jax.vjp(lambda a, b: excited(a, b, w_squeeze, w_excite), own, squeezed)
    field_grad, d_squeezed = back(d_weighted)
    field_grad = field_grad + (d_squeezed * (1.0 / width))[:, None, :]

    high_low = parts[:, LIMIT * width : LIMIT * width + 2 * each // samples].astype(f32)
    piece = jnp.sum(high_low, axis=0)
    piece = piece[: each // samples] + piece[each // samples :]
    piece = jnp.sum(spread(piece, "sub", subs), axis=0) * (1.0 / total_samples)
    piece = jnp.concatenate(halves(piece), axis=0)

    slot_count = per_owner * tables
    onehot = (slot_index[None, :] == jnp.arange(slot_count, dtype=jnp.int32)[:, None]).astype(bf16)
    placed = jnp.einsum(
        "sf,fen->sen", onehot, field_grad.astype(bf16), preferred_element_type=f32
    ).astype(bf16)
    placed = placed.reshape(tables, per_owner * width, samples)
    placed = jnp.concatenate(
        [placed, jnp.broadcast_to(piece[None], (tables, *piece.shape))], axis=1
    )
    placed = lax.all_to_all(placed, "table", split_axis=0, concat_axis=0, tiled=True)
    row_grads = placed[:, : per_owner * width].reshape(tables, per_owner, 1, width, samples)
    row_grads = jnp.moveaxis(row_grads, 1, 0)
    whole = placed[:, per_owner * width :].astype(f32)
    whole = (whole[:, : each // samples] + whole[:, each // samples :]).reshape(-1)
    ends = np.cumsum([w_excite.size, w_squeeze.size, w_bilinear.size])
    g_excite = whole[: ends[0]].reshape(w_excite.shape)
    g_squeeze = whole[ends[0] : ends[1]].reshape(w_squeeze.shape)
    g_bilinear = whole[ends[1] : ends[2]].reshape(w_bilinear.shape)
    return (row_grads, weight_grad, g_squeeze, g_excite, g_bilinear)


def solution(mesh):
    return jax.shard_map(
        on_device,
        mesh=mesh,
        in_specs=(
            P("table", None, "sub", None, None),
            P(),
            P(),
            P(),
            P(),
            P(BOTH, None),
            P(None, BOTH),
        ),
        out_specs=(P("table", None, "sub", None, None), P(BOTH, None), P(), P(), P()),
        check_vma=False,
    )
```

```python
import functools

import jax
import jax.numpy as jnp
import numpy as np
from jax import lax
from jax.experimental import pallas as pl
from jax.experimental.pallas import tpu as pltpu
from jax.sharding import PartitionSpec as P


HIGH = lax.Precision.HIGHEST
BOTH = ("table", "sub")
PLANES = 4
LIMIT = 13

WORKER = (
    4, 3, 2, 5, 0, 2, 4, 3, 7, 3, 0, 4, 6, 2, 2, 6, 6, 3, 4, 0, 3, 7, 1, 1, 5, 7, 6, 0, 5, 6, 7, 1, 2, 1, 5, 5, 1, 4, 3, 2, 2, 4, 7, 7, 0, 1, 5,
    5, 0, 6, 1, 6, 4, 3, 7, 3, 0, 4, 6, 2, 2, 1, 6, 3, 4, 0, 3, 0, 2, 1, 6, 7, 6, 0, 5, 6, 7, 1, 2, 1, 5, 5, 1, 4, 3, 2, 2, 4, 7, 7, 0, 1, 5, 1,
    5, 4, 3, 4, 3, 7, 3, 0, 4, 6, 2, 2, 6, 6, 3, 4, 0, 3, 7, 2, 1, 6, 7, 6, 0, 5, 6, 7, 1, 2, 1, 5, 5, 1, 4, 3, 2, 2, 4, 5, 7, 0, 1, 5, 7, 3, 4,
    4, 3, 7, 3, 0, 4, 6, 2, 2, 6, 6, 3, 4, 0, 3, 0, 1, 1, 5, 7, 6, 0, 5, 6, 7, 1, 2, 1, 5, 5, 1, 4, 3, 2, 2, 4, 5, 7, 0, 5, 5, 1, 7, 4, 3, 7, 3,
    0, 4, 6, 2, 2, 6, 6, 3, 4, 0, 3, 0, 2, 1, 5, 7, 6, 0, 5, 6, 7, 1, 2, 1, 5, 5, 1, 4, 3, 2, 2, 4, 5, 7, 0, 5, 5, 0, 4, 3, 7, 3, 0, 4, 6, 2, 2,
    6, 6, 3, 4, 0, 3, 7, 2, 1, 6, 7, 6, 0, 5, 6, 7, 1, 2, 1, 5, 5, 1, 4, 3, 2, 2, 4, 7, 7, 0, 5, 5, 4, 3, 7, 3, 0, 4, 6, 2, 2, 6, 6, 3, 4, 0, 3,
    1, 5, 7, 6, 6, 4, 0, 1, 5, 2, 1, 4, 7, 0, 6, 0, 6, 3, 4, 7, 1, 7, 3, 0, 3, 5, 6, 0, 2, 3, 2, 4, 3, 2, 4, 1, 5, 3, 2, 2, 1, 5, 7, 6, 6, 4, 0,
    1, 5, 2, 1, 4, 7, 0, 6, 0, 6, 3, 4, 7, 1, 7, 3, 0, 3, 5, 7, 4, 3, 6, 5, 3, 2, 4, 1, 5, 3, 2, 2, 1, 5, 7, 6, 6, 4, 2, 1, 5, 2, 1, 4, 7, 0, 6,
    0, 6, 3, 4, 7, 1, 7, 6, 0, 3, 5, 7, 0, 3, 5, 3, 2, 4, 1, 5, 3, 2, 2, 1, 5, 7, 0, 6, 4, 2, 1, 5, 2, 1, 4, 7, 0, 6, 0, 6, 3, 4, 7, 1, 7, 3, 0,
    3, 5, 3, 7, 5, 3, 2, 4, 1, 5, 3, 2, 2, 1, 5, 7, 0, 6, 4, 2, 1, 5, 2, 1, 4, 7, 0, 6, 0, 6, 3, 4, 7, 1, 7, 6, 0, 3, 5, 5, 4, 3, 2, 4, 1, 5, 3,
    2, 2, 1, 5, 7, 0, 6, 4, 0, 1, 5, 2, 1, 4, 7, 0, 6, 0, 6, 3, 4, 7, 1, 7, 3, 0, 3, 5, 2, 3, 2, 4, 1, 5, 3, 2, 2, 1, 5, 7, 0, 6, 4, 0, 1, 5, 2,
    1, 4, 7, 0, 6, 0, 6, 3, 4, 7, 1, 7, 6, 0, 3, 5, 3, 2, 4, 1, 5, 3, 2, 2, 1, 5, 7, 0, 6, 4, 2, 1, 5, 2, 1, 4, 7, 0, 6, 0, 6, 3, 4, 7, 1, 7, 6,
    0, 0, 0, 4, 2, 7, 7, 3, 5, 6, 4, 2, 5, 1, 3, 6, 1, 6, 7, 3, 4, 3, 1, 1, 4, 5, 7, 6, 1, 2, 4, 5, 7, 5, 2, 2, 4, 0, 0, 2, 0, 6, 1, 3, 5, 1, 3,
    6, 1, 6, 7, 3, 4, 3, 1, 5, 4, 5, 7, 6, 2, 0, 4, 1, 7, 5, 0, 2, 4, 3, 7, 3, 1, 1, 6, 0, 1, 3, 6, 2, 6, 7, 3, 4, 3, 2, 1, 4, 0, 7, 6, 2, 0, 4,
    1, 7, 0, 2, 2, 0, 7, 3, 4, 4, 6, 5, 5, 3, 6, 2, 6, 7, 3, 4, 3, 2, 5, 4, 0, 7, 6, 2, 0, 4, 5, 7, 5, 2, 0, 7, 0, 1, 4, 4, 0, 1, 3, 6, 1, 6, 7,
    3, 4, 3, 1, 1, 4, 0, 7, 6, 1, 0, 4, 1, 7, 0, 0, 0, 6, 2, 7, 2, 5, 5, 3, 6, 2, 6, 7, 3, 4, 3, 2, 5, 4, 5, 7, 6, 2, 2, 4, 5, 7, 5, 2, 2, 3, 0,
    6, 5, 1, 3, 6, 1, 6, 7, 3, 4, 3, 1, 1, 4, 0, 7, 6, 1, 0, 4, 5, 7, 0, 0, 0, 3, 4, 5, 1, 3, 6, 2, 6, 7, 3, 4, 3, 1, 5, 4, 5, 7, 6, 2, 2, 4, 5,
    7, 5, 2, 2, 7, 0, 1, 3, 6, 1, 6, 7, 3, 4, 3, 1, 1, 4, 0, 7, 6, 1, 0, 4, 1, 7, 0, 0, 0, 5, 5, 3, 6, 2, 6, 7, 3, 4, 3, 2, 5, 4, 5, 7, 6, 2, 2,
    6, 6, 6, 1, 1, 1, 3, 5, 7, 5, 7, 0, 7, 0, 5, 0, 2, 3, 0, 5, 2, 0, 2, 5, 7, 3, 2, 7, 3, 3, 4, 2, 4, 1, 1, 4, 1, 3, 2, 3, 4, 2, 2, 4, 2, 4, 4,
    3, 2, 1, 1, 0, 6, 7, 5, 0, 0, 7, 3, 6, 6, 7, 5, 0, 5, 6, 7, 5, 6, 3, 7, 3, 6, 4, 6, 7, 3, 7, 0, 6, 7, 4, 3, 3, 0, 0, 4, 6, 4, 4, 7, 3, 1, 1,
    5, 2, 1, 2, 6, 1, 5, 2, 2, 1, 2, 5, 5, 6, 2, 6, 5, 1, 7, 4, 1, 4, 2, 7, 4, 2, 7, 1, 2, 4, 2, 7, 4, 7, 1, 5, 3, 0, 3, 6, 3, 0, 3, 0, 1, 6, 5,
    6, 6, 1, 6, 6, 5, 7, 4, 4, 1, 7, 5, 0, 1, 0, 7, 5, 7, 4, 7, 1, 5, 0, 2, 3, 5, 2, 3, 4, 0, 4, 2, 0, 3, 2, 3, 0, 1, 7, 5, 5, 7, 5, 0, 5, 5, 7,
    1, 1, 1, 2, 3, 4, 3, 0, 4, 0, 4, 4, 0, 3, 2, 3, 6, 4, 2, 2, 1, 6, 6, 6, 4, 2, 1, 1, 7, 3, 3, 1, 6, 6, 6, 3, 1, 6, 1, 5, 7, 0, 0, 4, 4, 4, 4,
    7, 5, 3, 5, 2, 5, 2, 3, 2, 2, 5, 0, 0, 7, 2, 3, 2, 2, 3, 0, 4, 5, 0, 1, 1, 5, 6, 6, 0, 2, 2, 6, 5, 6, 4, 7, 5, 7, 4, 7, 5, 3, 7, 3, 1, 1, 6,
)


@functools.lru_cache(maxsize=None)
def make_plan(count, tables, subs, width, rows):
    plane = tables // PLANES
    held = rows * subs
    unit = 8
    assert width % unit == 0 and held % unit == 0
    pairs = [(i, j) for i in range(count) for j in range(i + 1, count)]
    assert len(pairs) == len(WORKER) and len(pairs) * width == held * tables
    per_plane = len(pairs) // PLANES
    worker = [plane * (g // per_plane) + WORKER[g] for g in range(len(pairs))]
    fields = [set() for _ in range(tables)]
    for g, r in enumerate(worker):
        fields[r] |= set(pairs[g])
    fields = [sorted(s) for s in fields]
    assert max(len(s) for s in fields) <= LIMIT
    table = np.zeros((tables, LIMIT), np.int32)
    live = np.zeros((tables, LIMIT), bool)
    for r, s in enumerate(fields):
        table[r, : len(s)] = s
        live[r, : len(s)] = True
    touched = [[[] for _ in range(plane)] for _ in range(tables)]
    for t in range(tables):
        for g in range(held * t // width, (held * (t + 1) - 1) // width + 1):
            assert worker[g] // plane == t // plane
            touched[t][worker[g] % plane].append(g)
    depth = max(len(x) for y in touched for x in y)
    units = held // unit
    per = width // unit
    pick = np.full((tables, plane, depth, per), units, np.int32)
    back = np.zeros((tables, units), np.int32)
    left = np.zeros((tables, plane * depth), np.int32)
    right = np.zeros((tables, plane * depth), np.int32)
    for t in range(tables):
        for w in range(plane):
            for c, g in enumerate(touched[t][w]):
                r = t // plane * plane + w
                k = (t % plane) ^ w
                slot = k * depth + c
                left[r, slot] = fields[r].index(pairs[g][0])
                right[r, slot] = fields[r].index(pairs[g][1])
                for q in range(per):
                    u = (width * g - held * t) // unit + q
                    if 0 <= u < units:
                        pick[t, k, c, q] = u
                        back[t, u] = (k * depth + c) * per + q
    return dict(
        table=table, live=live, depth=depth, pick=pick.reshape(tables, -1), back=back,
        left=left, right=right, plane=plane, unit=unit, units=units,
    )


def hadamard_np(width):
    index = np.arange(width)
    both = index[:, None] & index[None, :]
    parity = np.zeros((width, width), int)
    for bit_pos in range(width.bit_length()):
        parity = parity ^ (both >> bit_pos & 1)
    return (1 - 2 * parity).astype(np.float32)


def slot_table(field_owner, per_owner):
    count = field_owner.shape[0]
    order = jnp.arange(count, dtype=jnp.int32)
    same = field_owner[:, None] == field_owner[None, :]
    earlier = order[:, None] > order[None, :]
    position = jnp.sum((same & earlier).astype(jnp.int32), axis=1)
    return field_owner * per_owner + position


def swap(value, axis, size, k):
    return lax.ppermute(value, axis, [(a, a ^ k) for a in range(size)])


def trade(blocks, axis, size):
    return [blocks[0]] + [swap(b, axis, size, k) for k, b in enumerate(blocks) if k]


def xor_order(blocks, axis):
    own = lax.axis_index(axis)
    return jnp.take(blocks, own ^ jnp.arange(blocks.shape[0], dtype=jnp.int32), axis=0, mode="clip")


def halves(x):
    high = x.astype(jnp.bfloat16)
    return high, (x - high.astype(jnp.float32)).astype(jnp.bfloat16)


def pack_rows(received, squeezed, slot_index, table):
    slots, width, samples = received.shape
    count = squeezed.shape[0]
    tables = table.shape[0] // LIMIT
    total = LIMIT * width + count
    turn = 8

    def body(slot_ref, table_ref, received_ref, squeezed_ref, out_ref):
        first = pl.program_id(0) * (turn * LIMIT)
        for r in range(turn):
            for k in range(LIMIT):
                out_ref[r, k * width : (k + 1) * width, :] = received_ref[
                    slot_ref[table_ref[first + r * LIMIT + k]]
                ]
            out_ref[r, LIMIT * width :, :] = squeezed_ref[...]

    return pl.pallas_call(
        body,
        out_shape=jax.ShapeDtypeStruct((tables, total, samples), received.dtype),
        grid_spec=pltpu.PrefetchScalarGridSpec(
            num_scalar_prefetch=2,
            grid=(tables // turn,),
            in_specs=[
                pl.BlockSpec((slots, width, samples), lambda i, *_: (0, 0, 0)),
                pl.BlockSpec((count, samples), lambda i, *_: (0, 0)),
            ],
            out_specs=pl.BlockSpec((turn, total, samples), lambda i, *_: (i, 0, 0)),
        ),
        name="pack_rows",
    )(slot_index, table, received, squeezed)


def tower_pairs(own, pieces, cotangent):
    tall, quarter = pieces[0].shape
    hidden, cols = cotangent.shape
    parts = len(pieces)
    step = 512

    def body(own_ref, *refs):
        cot_ref, out_ref, rows_ref = refs[parts:]

        @pl.when(pl.program_id(0) == 0)
        def _():
            for o in range(parts):

                @pl.when(own_ref[0] == o)
                def _(o=o):
                    for q in range(parts):
                        rows_ref[:, q * quarter : (q + 1) * quarter] = refs[o ^ q][...]

        out_ref[...] = jnp.dot(
            rows_ref[...], cot_ref[...], preferred_element_type=jnp.float32
        ).astype(out_ref.dtype)

    return pl.pallas_call(
        body,
        out_shape=jax.ShapeDtypeStruct((tall, cols), cotangent.dtype),
        grid_spec=pltpu.PrefetchScalarGridSpec(
            num_scalar_prefetch=1,
            grid=(cols // step,),
            in_specs=[
                *[pl.BlockSpec((tall, quarter), lambda i, *_: (0, 0)) for _ in pieces],
                pl.BlockSpec((hidden, step), lambda i, *_: (0, i)),
            ],
            out_specs=pl.BlockSpec((tall, step), lambda i, *_: (0, i)),
            scratch_shapes=[pltpu.VMEM((tall, hidden), cotangent.dtype)],
        ),
        compiler_params=pltpu.CompilerParams(vmem_limit_bytes=40 * 1024 * 1024),
        cost_estimate=pl.CostEstimate(
            flops=2 * tall * hidden * cols, transcendentals=0, bytes_accessed=30_000_000
        ),
        name="tower_pairs",
    )(own, *pieces, cotangent)


def owner_step(parts, selected, squeezed, table, slot_index, w_ex, w_ext, w_sq, w_sqt, slots):
    tables, span, samples = parts.shape
    count, width, _ = selected.shape
    scale = 1.0 / width**0.5
    f32, bf16 = jnp.float32, jnp.bfloat16
    turn = 8
    bundle = 8

    def dot(a, b):
        return jnp.dot(a, b, preferred_element_type=f32)

    def body(table_ref, slot_ref, parts_ref, sel_ref, sq_ref, hd_ref, wex_ref, wext_ref, wsq_ref,
             wsqt_ref, out_ref, acc, ex, sp):
        step = pl.program_id(0)

        @pl.when(step == 0)
        def _():
            acc[...] = jnp.zeros_like(acc)

        for r in range(turn):
            for k in range(LIMIT):
                f = table_ref[(step * turn + r) * LIMIT + k]
                acc[f] += parts_ref[r, k * width : (k + 1) * width, :].astype(f32)

        @pl.when(step == pl.num_programs(0) - 1)
        def _():
            sq = sq_ref[...]
            pre = dot(wsq_ref[...], jnp.concatenate([sq, sq, sq], axis=0)) * scale
            gate = 1.0 / (1.0 + jnp.exp(-pre))
            ah, al = halves(pre * gate)
            ex[...] = dot(wex_ref[...], jnp.concatenate([ah, ah, al], axis=0))
            d_act = jnp.zeros(pre.shape, f32)
            for b in range(count // bundle):
                at = slice(b * bundle * width, (b + 1) * bundle * width)
                rows = sel_ref[b * bundle : (b + 1) * bundle].reshape(bundle * width, samples)
                fields = dot(hd_ref[...], rows) * scale
                got = acc[b * bundle : (b + 1) * bundle].reshape(bundle * width, samples)
                eh, el = halves(got * fields)
                d_act = d_act + dot(wext_ref[b, 0], eh) + dot(wext_ref[b, 0], el)
                d_act = d_act + dot(wext_ref[b, 1], eh)
                ex[at] = got * (1.0 + ex[at])
            d_pre = d_act * gate * (1.0 + pre * (1.0 - gate))
            ph, pl_ = halves(d_pre)
            sp[...] = dot(wsqt_ref[...], jnp.concatenate([ph, pl_, ph], axis=0)) * (1.0 / width)
            out_ref[...] = jnp.zeros_like(out_ref)
            for f in range(count):
                grad = ex[f * width : (f + 1) * width] + sp[f : f + 1, :]
                out_ref[slot_ref[f]] = grad.astype(bf16)

    hd = jnp.asarray(np.kron(np.eye(bundle), hadamard_np(width)), bf16)
    mats = (selected, squeezed, hd, w_ex, w_ext, w_sq, w_sqt)
    return pl.pallas_call(
        body,
        out_shape=jax.ShapeDtypeStruct((slots, width, samples), bf16),
        grid_spec=pltpu.PrefetchScalarGridSpec(
            num_scalar_prefetch=2,
            grid=(tables // turn,),
            in_specs=[
                pl.BlockSpec((turn, span, samples), lambda i, *_: (i, 0, 0)),
                *[pl.BlockSpec(m.shape, lambda i, *_, n=m.ndim: (0,) * n) for m in mats],
            ],
            out_specs=pl.BlockSpec((slots, width, samples), lambda i, *_: (0, 0, 0)),
            scratch_shapes=[
                pltpu.VMEM((count, width, samples), f32),
                pltpu.VMEM((count * width, samples), f32),
                pltpu.VMEM((count, samples), f32),
            ],
        ),
        compiler_params=pltpu.CompilerParams(vmem_limit_bytes=40 * 1024 * 1024),
        name="owner_step",
    )(table, slot_index, parts, *mats)


def pair_step(got, pair_grad, left, right, signs, w_pairs, w_ex, w_ext, w_sq, width):
    tables, tall, samples = got.shape
    slots = left.shape[0]
    units = w_sq.shape[0]
    count = tall - LIMIT * width
    span = LIMIT * width
    group = 4
    cols = group * samples
    scale = 1.0 / width**0.5
    f32, bf16 = jnp.float32, jnp.bfloat16

    def dot(a, b):
        return jnp.dot(a, b, preferred_element_type=f32)

    def dot_nt(a, b):
        return lax.dot_general(a, b, (((1,), (1,)), ((), ())), preferred_element_type=f32)

    half = (LIMIT + 1) // 2 * width
    spans = [slice(0, half), slice(half, span)]

    def blocks(a, b):
        return jnp.concatenate([dot(a[s, : s.stop - s.start], b[s]) for s in spans], axis=0)

    def body(left_ref, right_ref, got_ref, pg_ref, hd_ref, rep_ref, rept_ref, mask_ref, wb_ref,
             wex_ref, wext_ref, wsq_ref, pairs_ref, part_ref, dbil_ref, dex_ref, dsq_ref,
             wt, mp, dm, dw, mats):
        @pl.when(pl.program_id(0) == 0)
        def _():
            for k in range(4):
                tall = dot(rep_ref[...], wb_ref[k]).astype(bf16)
                mats[k] = (dot(tall, rept_ref[...]) * mask_ref[...]).astype(bf16)
            dbil_ref[...] = jnp.zeros_like(dbil_ref)
            dex_ref[...] = jnp.zeros_like(dex_ref)
            dsq_ref[...] = jnp.zeros_like(dsq_ref)

        rows = jnp.concatenate([got_ref[o] for o in range(group)], axis=1)
        sq = rows[span:]
        fields = blocks(hd_ref, rows[:span]) * scale
        pre = dot(wsq_ref[...], jnp.concatenate([sq, sq, sq], axis=0)) * scale
        gate = 1.0 / (1.0 + jnp.exp(-pre))
        act = pre * gate
        ah, al = halves(act)
        excite = dot(wex_ref[...], jnp.concatenate([ah, ah, al], axis=0))
        weighted = fields * (1.0 + excite)
        wh, wl = halves(weighted)
        mapped = blocks(mats.at[0], wh) + blocks(mats.at[0], wl) + blocks(mats.at[1], wh)
        wt[...] = weighted.reshape(LIMIT, width, cols)
        mp[...] = mapped.reshape(LIMIT, width, cols)
        dm[...] = jnp.zeros_like(dm)
        dw[...] = jnp.zeros_like(dw)

        def one(p, carry):
            i = left_ref[p]
            j = right_ref[p]
            off = pl.multiple_of(p * width, width)
            x = mp[i]
            y = wt[j]
            pairs_ref[pl.ds(off, width), :] = (x * y).astype(bf16)
            g = pg_ref[pl.ds(off, width), :].astype(f32)
            dm[i] += g * y
            dw[j] += g * x
            return carry

        lax.fori_loop(0, slots, one, 0, unroll=2)
        dmv = dm[...].reshape(span, cols)
        dh, dl = halves(dmv)
        part = dw[...].reshape(span, cols) + (
            blocks(mats.at[2], dh) + blocks(mats.at[2], dl) + blocks(mats.at[3], dh)
        )
        sent = part.astype(bf16)
        for o in range(group):
            part_ref[o] = sent[:, o * samples : (o + 1) * samples]
        d_excite = part * fields
        eh, el = halves(d_excite)
        d_act = dot(wext_ref[...], jnp.concatenate([eh, el, eh], axis=0))
        d_pre = d_act * gate * (1.0 + pre * (1.0 - gate))
        ph, pl_ = halves(d_pre)

        for s in spans:
            dbil_ref[s, : s.stop - s.start] += dot_nt(wh[s], dh[s])
        dex_ref[...] += dot_nt(jnp.concatenate([ah, al], axis=0), eh)
        dsq_ref[...] += dot_nt(jnp.concatenate([ph, pl_], axis=0), sq)

    def whole(a):
        return pl.BlockSpec(a.shape, lambda i, *_, n=a.ndim: (0,) * n)

    block = np.kron(np.eye(LIMIT), np.ones((width, width)))
    turned = np.zeros((span, half), np.float32)
    mask = np.zeros((span, half), np.float32)
    for s in spans:
        turned[s, : s.stop - s.start] = np.kron(np.eye(LIMIT), signs)[s, s]
        mask[s, : s.stop - s.start] = block[s, s]
    repeat = np.tile(np.eye(width), (LIMIT, 1))
    mats = (
        jnp.asarray(turned, bf16),
        jnp.asarray(repeat, bf16),
        jnp.asarray(repeat[:half].T, bf16),
        jnp.asarray(mask, f32),
        w_pairs,
        w_ex,
        w_ext,
        w_sq,
    )
    return pl.pallas_call(
        body,
        out_shape=(
            jax.ShapeDtypeStruct((slots * width, tables * samples), bf16),
            jax.ShapeDtypeStruct((tables, span, samples), bf16),
            jax.ShapeDtypeStruct((span, half), f32),
            jax.ShapeDtypeStruct((2 * units, span), f32),
            jax.ShapeDtypeStruct((2 * units, count), f32),
        ),
        grid_spec=pltpu.PrefetchScalarGridSpec(
            num_scalar_prefetch=2,
            grid=(tables // group,),
            in_specs=[
                pl.BlockSpec((group, got.shape[1], samples), lambda i, *_: (i, 0, 0)),
                pl.BlockSpec((slots * width, cols), lambda i, *_: (0, i)),
                *[whole(m) for m in mats],
            ],
            out_specs=[
                pl.BlockSpec((slots * width, cols), lambda i, *_: (0, i)),
                pl.BlockSpec((group, span, samples), lambda i, *_: (i, 0, 0)),
                pl.BlockSpec((span, half), lambda i, *_: (0, 0)),
                pl.BlockSpec((2 * units, span), lambda i, *_: (0, 0)),
                pl.BlockSpec((2 * units, count), lambda i, *_: (0, 0)),
            ],
            scratch_shapes=[
                *[pltpu.VMEM((LIMIT, width, cols), f32) for _ in range(4)],
                pltpu.VMEM((4, span, half), bf16),
            ],
        ),
        compiler_params=pltpu.CompilerParams(vmem_limit_bytes=40 * 1024 * 1024),
        name="pair_step",
    )(left, right, got, pair_grad, *mats)


def on_device(pooled, field_owner, w_squeeze, w_excite, w_bilinear, tower_weight, tower_cotangent):
    f32, bf16 = jnp.float32, jnp.bfloat16
    per_owner, _, _, width, samples = pooled.shape
    tables, subs = lax.axis_size("table"), lax.axis_size("sub")
    total_samples = tables * subs * samples
    count = field_owner.shape[0]
    rows, hidden = tower_weight.shape
    plan = make_plan(count, tables, subs, width, rows)
    plane, depth, unit, units = plan["plane"], plan["depth"], plan["unit"], plan["units"]
    quarter = hidden // subs
    scale = 1.0 / width**0.5
    signs_np = hadamard_np(width)
    signs = jnp.asarray(signs_np, bf16)
    here = lax.axis_index("table")

    rotated = (
        jnp.einsum("ij,ktsjb->ktsib", signs, pooled, preferred_element_type=f32) * scale
    ).astype(bf16)
    rotated, tower_weight = lax.optimization_barrier((rotated, tower_weight))
    received = lax.all_to_all(rotated, "table", split_axis=1, concat_axis=0, tiled=True)
    received = received.reshape(per_owner * tables, width, samples)

    cut = jnp.moveaxis(tower_weight.reshape(rows, subs, quarter), 1, 0)
    cut = xor_order(cut, "sub")
    cut = trade([cut[k] for k in range(subs)], "sub", subs)

    slot_index = slot_table(field_owner, per_owner)
    table = jnp.asarray(plan["table"].reshape(-1))
    selected = jnp.take(received, slot_index, axis=0, mode="clip")
    squeeze_rows = selected[:, 0, :]

    cut = xor_order(jnp.stack(cut), "sub").reshape(units, unit, quarter)
    cut = jnp.concatenate([cut, jnp.zeros((1, unit, quarter), bf16)], axis=0)
    cut = jnp.take(cut, jnp.asarray(plan["pick"])[here], axis=0, mode="clip")
    cut = cut.reshape(plane, depth * width, quarter)
    cut = trade([cut[k] for k in range(plane)], "table", tables)
    cut = jnp.concatenate(cut, axis=0)

    sent = pack_rows(received, squeeze_rows, slot_index, table)
    sent, cut = lax.optimization_barrier((sent, cut))
    got = lax.all_to_all(sent, "table", split_axis=0, concat_axis=0, tiled=True)
    pieces = trade([cut] * subs, "sub", subs)

    cotangent = lax.all_gather(tower_cotangent, "table", axis=1, tiled=True)
    own_sub = lax.axis_index("sub")
    pair_grad = tower_pairs(own_sub[None], pieces, cotangent)

    xh, xl = halves(w_excite)
    mine = jnp.asarray(plan["table"])[here]
    here_h, here_l = [
        jnp.take(x.reshape(count, width, -1), mine, axis=0, mode="clip").reshape(LIMIT * width, -1)
        for x in (xh, xl)
    ]
    s1, s2 = halves(w_squeeze)
    s3 = (w_squeeze - s1.astype(f32) - s2.astype(f32)).astype(bf16)
    w_sq = jnp.concatenate([s1, s2, s3], axis=1)
    pairs, part, d_bilinear, d_excite, d_squeeze = pair_step(
        got,
        pair_grad,
        jnp.asarray(plan["left"])[here],
        jnp.asarray(plan["right"])[here],
        signs_np,
        jnp.stack([*halves(w_bilinear.T), *halves(w_bilinear)]),
        jnp.concatenate([here_h, here_l, here_h], axis=1),
        jnp.concatenate([here_h, here_h, here_l], axis=0).T,
        w_sq,
        width,
    )
    parts = lax.all_to_all(part, "table", split_axis=0, concat_axis=0, tiled=True)

    total = lax.dot_general(
        pairs, cotangent, (((1,), (1,)), ((), ())), preferred_element_type=f32
    )
    total = jnp.moveaxis(total.astype(bf16).reshape(-1, subs, quarter), 1, 0)
    total = xor_order(total, "sub")
    total = trade([total[k] for k in range(subs)], "sub", subs)
    total = sum(x.astype(f32) for x in total) * (1.0 / total_samples)
    total = total.astype(bf16).reshape(plane, depth * width, quarter)
    total = trade([total[k] for k in range(plane)], "table", tables)
    total = jnp.concatenate(total, axis=0).reshape(-1, unit, quarter)
    total = jnp.take(total, jnp.asarray(plan["back"])[here], axis=0, mode="clip")
    total = xor_order(total.reshape(subs, rows, quarter), "sub")
    total = trade([total[k] for k in range(subs)], "sub", subs)
    total = xor_order(jnp.stack(total), "sub")
    weight_grad = jnp.moveaxis(total, 0, 1).reshape(rows, hidden).astype(f32)

    hidden_units = w_squeeze.shape[0]
    half = d_bilinear.shape[1]
    d_bilinear = sum(
        d_bilinear[k : k + width, k % half : k % half + width]
        for k in range(0, LIMIT * width, width)
    )
    d_excite = d_excite[:hidden_units] + d_excite[hidden_units:]
    d_squeeze = (d_squeeze[:hidden_units] + d_squeeze[hidden_units:]) * scale
    lift = (jnp.arange(count, dtype=jnp.int32)[:, None] == mine[None, :]) & jnp.asarray(
        plan["live"]
    )[here][None, :]
    d_excite = d_excite.reshape(hidden_units, LIMIT, width).transpose(1, 2, 0)
    d_excite = jnp.dot(
        lift.astype(f32), d_excite.reshape(LIMIT, width * hidden_units), precision=HIGH
    )
    small = jnp.concatenate([d_excite.reshape(-1), d_squeeze.reshape(-1), d_bilinear.reshape(-1)])
    ends = np.cumsum([w_excite.size, w_squeeze.size, w_bilinear.size])
    small = jnp.pad(small, (0, -small.size % 1024)).reshape(-1, 128)
    for axis, size in (("table", tables), ("sub", subs)):
        bit = 1
        while bit < size:
            small = small + swap(small, axis, size, bit)
            bit *= 2
    small = small.reshape(-1) * (1.0 / total_samples)
    g_excite = small[: ends[0]].reshape(w_excite.shape)
    g_squeeze = small[ends[0] : ends[1]].reshape(w_squeeze.shape)
    g_bilinear = small[ends[1] : ends[2]].reshape(w_bilinear.shape)

    bundled = [x.T.reshape(hidden_units, count // 8, 8 * width).transpose(1, 0, 2) for x in (xh, xl)]
    placed = owner_step(
        parts,
        selected,
        squeeze_rows,
        table,
        slot_index,
        jnp.concatenate([xh, xl, xh], axis=1),
        jnp.stack(bundled, axis=1),
        w_sq,
        jnp.concatenate([s1, s1, s2], axis=0).T,
        per_owner * tables,
    )
    placed = placed.reshape(per_owner * tables, 1, 1, width, samples)
    row_grads = lax.all_to_all(placed, "table", split_axis=0, concat_axis=1, tiled=True)
    return (row_grads, weight_grad, g_squeeze, g_excite, g_bilinear)


def solution(mesh):
    return jax.shard_map(
        on_device,
        mesh=mesh,
        in_specs=(
            P("table", None, "sub", None, None),
            P(),
            P(),
            P(),
            P(),
            P(BOTH, None),
            P(None, BOTH),
        ),
        out_specs=(P("table", None, "sub", None, None), P(BOTH, None), P(), P(), P()),
        check_vma=False,
    )
```

```python
import functools

import jax
import jax.numpy as jnp
import numpy as np
from jax import lax
from jax.experimental import pallas as pl
from jax.experimental.pallas import tpu as pltpu
from jax.sharding import PartitionSpec as P


HIGH = lax.Precision.HIGHEST
BOTH = ("table", "sub")
PLANES = 4
LIMIT = 13

WORKER = (
    4, 3, 2, 5, 0, 2, 4, 3, 7, 3, 0, 4, 6, 2, 2, 6, 6, 3, 4, 0, 3, 7, 1, 1, 5, 7, 6, 0, 5, 6, 7, 1, 2, 1, 5, 5, 1, 4, 3, 2, 2, 4, 7, 7, 0, 1, 5,
    5, 0, 6, 1, 6, 4, 3, 7, 3, 0, 4, 6, 2, 2, 1, 6, 3, 4, 0, 3, 0, 2, 1, 6, 7, 6, 0, 5, 6, 7, 1, 2, 1, 5, 5, 1, 4, 3, 2, 2, 4, 7, 7, 0, 1, 5, 1,
    5, 4, 3, 4, 3, 7, 3, 0, 4, 6, 2, 2, 6, 6, 3, 4, 0, 3, 7, 2, 1, 6, 7, 6, 0, 5, 6, 7, 1, 2, 1, 5, 5, 1, 4, 3, 2, 2, 4, 5, 7, 0, 1, 5, 7, 3, 4,
    4, 3, 7, 3, 0, 4, 6, 2, 2, 6, 6, 3, 4, 0, 3, 0, 1, 1, 5, 7, 6, 0, 5, 6, 7, 1, 2, 1, 5, 5, 1, 4, 3, 2, 2, 4, 5, 7, 0, 5, 5, 1, 7, 4, 3, 7, 3,
    0, 4, 6, 2, 2, 6, 6, 3, 4, 0, 3, 0, 2, 1, 5, 7, 6, 0, 5, 6, 7, 1, 2, 1, 5, 5, 1, 4, 3, 2, 2, 4, 5, 7, 0, 5, 5, 0, 4, 3, 7, 3, 0, 4, 6, 2, 2,
    6, 6, 3, 4, 0, 3, 7, 2, 1, 6, 7, 6, 0, 5, 6, 7, 1, 2, 1, 5, 5, 1, 4, 3, 2, 2, 4, 7, 7, 0, 5, 5, 4, 3, 7, 3, 0, 4, 6, 2, 2, 6, 6, 3, 4, 0, 3,
    1, 5, 7, 6, 6, 4, 0, 1, 5, 2, 1, 4, 7, 0, 6, 0, 6, 3, 4, 7, 1, 7, 3, 0, 3, 5, 6, 0, 2, 3, 2, 4, 3, 2, 4, 1, 5, 3, 2, 2, 1, 5, 7, 6, 6, 4, 0,
    1, 5, 2, 1, 4, 7, 0, 6, 0, 6, 3, 4, 7, 1, 7, 3, 0, 3, 5, 7, 4, 3, 6, 5, 3, 2, 4, 1, 5, 3, 2, 2, 1, 5, 7, 6, 6, 4, 2, 1, 5, 2, 1, 4, 7, 0, 6,
    0, 6, 3, 4, 7, 1, 7, 6, 0, 3, 5, 7, 0, 3, 5, 3, 2, 4, 1, 5, 3, 2, 2, 1, 5, 7, 0, 6, 4, 2, 1, 5, 2, 1, 4, 7, 0, 6, 0, 6, 3, 4, 7, 1, 7, 3, 0,
    3, 5, 3, 7, 5, 3, 2, 4, 1, 5, 3, 2, 2, 1, 5, 7, 0, 6, 4, 2, 1, 5, 2, 1, 4, 7, 0, 6, 0, 6, 3, 4, 7, 1, 7, 6, 0, 3, 5, 5, 4, 3, 2, 4, 1, 5, 3,
    2, 2, 1, 5, 7, 0, 6, 4, 0, 1, 5, 2, 1, 4, 7, 0, 6, 0, 6, 3, 4, 7, 1, 7, 3, 0, 3, 5, 2, 3, 2, 4, 1, 5, 3, 2, 2, 1, 5, 7, 0, 6, 4, 0, 1, 5, 2,
    1, 4, 7, 0, 6, 0, 6, 3, 4, 7, 1, 7, 6, 0, 3, 5, 3, 2, 4, 1, 5, 3, 2, 2, 1, 5, 7, 0, 6, 4, 2, 1, 5, 2, 1, 4, 7, 0, 6, 0, 6, 3, 4, 7, 1, 7, 6,
    7, 7, 7, 4, 1, 1, 5, 6, 0, 4, 4, 5, 6, 5, 6, 2, 6, 0, 2, 3, 0, 2, 1, 4, 0, 5, 2, 3, 3, 5, 3, 1, 1, 2, 6, 3, 1, 4, 7, 6, 1, 5, 5, 2, 0, 5, 6,
    2, 6, 6, 0, 4, 2, 2, 1, 4, 0, 5, 2, 0, 0, 5, 4, 1, 1, 7, 7, 7, 4, 7, 6, 5, 4, 4, 3, 0, 5, 7, 4, 6, 6, 0, 3, 0, 7, 1, 3, 0, 5, 4, 3, 0, 5, 3,
    1, 1, 7, 7, 7, 1, 5, 1, 6, 4, 2, 6, 5, 6, 4, 6, 6, 2, 3, 2, 2, 1, 4, 3, 5, 2, 3, 3, 5, 4, 1, 1, 2, 6, 3, 7, 4, 1, 1, 5, 0, 5, 7, 4, 7, 0, 0,
    4, 0, 7, 1, 4, 0, 5, 4, 0, 0, 5, 4, 1, 1, 7, 7, 7, 6, 5, 7, 1, 6, 5, 6, 2, 6, 6, 2, 3, 2, 2, 1, 3, 3, 5, 2, 3, 3, 5, 3, 1, 1, 7, 6, 3, 2, 7,
    5, 6, 5, 6, 4, 7, 0, 2, 4, 0, 2, 1, 4, 0, 5, 4, 0, 0, 5, 4, 1, 1, 7, 7, 7, 1, 2, 6, 5, 6, 4, 6, 6, 2, 4, 2, 2, 1, 4, 3, 5, 4, 3, 3, 5, 3, 1,
    1, 2, 6, 3, 1, 0, 5, 7, 4, 7, 0, 0, 4, 0, 7, 1, 4, 0, 5, 4, 0, 0, 5, 4, 1, 1, 7, 7, 7, 6, 5, 6, 2, 6, 6, 2, 3, 2, 2, 1, 3, 3, 5, 2, 3, 3, 5,
    6, 6, 6, 1, 1, 1, 3, 5, 7, 5, 7, 0, 7, 0, 5, 0, 2, 3, 0, 5, 2, 0, 2, 5, 7, 3, 2, 7, 3, 3, 4, 2, 4, 1, 1, 4, 1, 3, 2, 3, 4, 2, 2, 4, 2, 4, 4,
    3, 2, 1, 1, 0, 6, 7, 5, 0, 0, 7, 3, 6, 6, 7, 5, 0, 5, 6, 7, 5, 6, 3, 7, 3, 6, 4, 6, 7, 3, 7, 0, 6, 7, 4, 3, 3, 0, 0, 4, 6, 4, 4, 7, 3, 1, 1,
    5, 2, 1, 2, 6, 1, 5, 2, 2, 1, 2, 5, 5, 6, 2, 6, 5, 1, 7, 4, 1, 4, 2, 7, 4, 2, 7, 1, 2, 4, 2, 7, 4, 7, 1, 5, 3, 0, 3, 6, 3, 0, 3, 0, 1, 6, 5,
    6, 6, 1, 6, 6, 5, 7, 4, 4, 1, 7, 5, 0, 1, 0, 7, 5, 7, 4, 7, 1, 5, 0, 2, 3, 5, 2, 3, 4, 0, 4, 2, 0, 3, 2, 3, 0, 1, 7, 5, 5, 7, 5, 0, 5, 5, 7,
    1, 1, 1, 2, 3, 4, 3, 0, 4, 0, 4, 4, 0, 3, 2, 3, 6, 4, 2, 2, 1, 6, 6, 6, 4, 2, 1, 1, 7, 3, 3, 1, 6, 6, 6, 3, 1, 6, 1, 5, 7, 0, 0, 4, 4, 4, 4,
    7, 5, 3, 5, 2, 5, 2, 3, 2, 2, 5, 0, 0, 7, 2, 3, 2, 2, 3, 0, 4, 5, 0, 1, 1, 5, 6, 6, 0, 2, 2, 6, 5, 6, 4, 7, 5, 7, 4, 7, 5, 3, 7, 3, 1, 1, 6,
)


@functools.lru_cache(maxsize=None)
def make_plan(count, tables, subs, width, rows):
    plane = tables // PLANES
    held = rows * subs
    unit = 8
    assert width % unit == 0 and held % unit == 0
    pairs = [(i, j) for i in range(count) for j in range(i + 1, count)]
    assert len(pairs) == len(WORKER) and len(pairs) * width == held * tables
    per_plane = len(pairs) // PLANES
    worker = [plane * (g // per_plane) + WORKER[g] for g in range(len(pairs))]
    fields = [set() for _ in range(tables)]
    for g, r in enumerate(worker):
        fields[r] |= set(pairs[g])
    fields = [sorted(s) for s in fields]
    assert max(len(s) for s in fields) <= LIMIT
    table = np.zeros((tables, LIMIT), np.int32)
    live = np.zeros((tables, LIMIT), bool)
    for r, s in enumerate(fields):
        table[r, : len(s)] = s
        live[r, : len(s)] = True
    touched = [[[] for _ in range(plane)] for _ in range(tables)]
    for t in range(tables):
        for g in range(held * t // width, (held * (t + 1) - 1) // width + 1):
            assert worker[g] // plane == t // plane
            touched[t][worker[g] % plane].append(g)
    depth = max(len(x) for y in touched for x in y)
    units = held // unit
    per = width // unit
    pick = np.full((tables, plane, depth, per), units, np.int32)
    back = np.zeros((tables, units), np.int32)
    left = np.zeros((tables, plane * depth), np.int32)
    right = np.zeros((tables, plane * depth), np.int32)
    for t in range(tables):
        for w in range(plane):
            for c, g in enumerate(touched[t][w]):
                r = t // plane * plane + w
                k = (t % plane) ^ w
                slot = k * depth + c
                left[r, slot] = fields[r].index(pairs[g][0])
                right[r, slot] = fields[r].index(pairs[g][1])
                for q in range(per):
                    u = (width * g - held * t) // unit + q
                    if 0 <= u < units:
                        pick[t, k, c, q] = u
                        back[t, u] = (k * depth + c) * per + q
    return dict(
        table=table, live=live, depth=depth, pick=pick.reshape(tables, -1), back=back,
        left=left, right=right, plane=plane, unit=unit, units=units,
    )


def hadamard_np(width):
    index = np.arange(width)
    both = index[:, None] & index[None, :]
    parity = np.zeros((width, width), int)
    for bit_pos in range(width.bit_length()):
        parity = parity ^ (both >> bit_pos & 1)
    return (1 - 2 * parity).astype(np.float32)


def slot_table(field_owner, per_owner):
    count = field_owner.shape[0]
    order = jnp.arange(count, dtype=jnp.int32)
    same = field_owner[:, None] == field_owner[None, :]
    earlier = order[:, None] > order[None, :]
    position = jnp.sum((same & earlier).astype(jnp.int32), axis=1)
    return field_owner * per_owner + position


def swap(value, axis, size, k):
    return lax.ppermute(value, axis, [(a, a ^ k) for a in range(size)])


def trade(blocks, axis, size):
    return [blocks[0]] + [swap(b, axis, size, k) for k, b in enumerate(blocks) if k]


def xor_order(blocks, axis):
    own = lax.axis_index(axis)
    return jnp.take(blocks, own ^ jnp.arange(blocks.shape[0], dtype=jnp.int32), axis=0, mode="clip")


def halves(x):
    high = x.astype(jnp.bfloat16)
    return high, (x - high.astype(jnp.float32)).astype(jnp.bfloat16)


def pack_rows(received, squeezed, slot_index, table):
    slots, width, samples = received.shape
    count = squeezed.shape[0]
    tables = table.shape[0] // LIMIT
    total = LIMIT * width + count
    turn = 8

    def body(slot_ref, table_ref, received_ref, squeezed_ref, out_ref):
        first = pl.program_id(0) * (turn * LIMIT)
        for r in range(turn):
            for k in range(LIMIT):
                out_ref[r, k * width : (k + 1) * width, :] = received_ref[
                    slot_ref[table_ref[first + r * LIMIT + k]]
                ]
            out_ref[r, LIMIT * width :, :] = squeezed_ref[...]

    return pl.pallas_call(
        body,
        out_shape=jax.ShapeDtypeStruct((tables, total, samples), received.dtype),
        grid_spec=pltpu.PrefetchScalarGridSpec(
            num_scalar_prefetch=2,
            grid=(tables // turn,),
            in_specs=[
                pl.BlockSpec((slots, width, samples), lambda i, *_: (0, 0, 0)),
                pl.BlockSpec((count, samples), lambda i, *_: (0, 0)),
            ],
            out_specs=pl.BlockSpec((turn, total, samples), lambda i, *_: (i, 0, 0)),
        ),
        name="pack_rows",
    )(slot_index, table, received, squeezed)


def tower_pairs(own, pieces, cotangent):
    tall, quarter = pieces[0].shape
    hidden, cols = cotangent.shape
    parts = len(pieces)
    step = 512

    def body(own_ref, *refs):
        cot_ref, out_ref, rows_ref = refs[parts:]

        @pl.when(pl.program_id(0) == 0)
        def _():
            for o in range(parts):

                @pl.when(own_ref[0] == o)
                def _(o=o):
                    for q in range(parts):
                        rows_ref[:, q * quarter : (q + 1) * quarter] = refs[o ^ q][...]

        out_ref[...] = jnp.dot(
            rows_ref[...], cot_ref[...], preferred_element_type=jnp.float32
        ).astype(out_ref.dtype)

    return pl.pallas_call(
        body,
        out_shape=jax.ShapeDtypeStruct((tall, cols), cotangent.dtype),
        grid_spec=pltpu.PrefetchScalarGridSpec(
            num_scalar_prefetch=1,
            grid=(cols // step,),
            in_specs=[
                *[pl.BlockSpec((tall, quarter), lambda i, *_: (0, 0)) for _ in pieces],
                pl.BlockSpec((hidden, step), lambda i, *_: (0, i)),
            ],
            out_specs=pl.BlockSpec((tall, step), lambda i, *_: (0, i)),
            scratch_shapes=[pltpu.VMEM((tall, hidden), cotangent.dtype)],
        ),
        compiler_params=pltpu.CompilerParams(vmem_limit_bytes=40 * 1024 * 1024),
        cost_estimate=pl.CostEstimate(
            flops=2 * tall * hidden * cols, transcendentals=0, bytes_accessed=30_000_000
        ),
        name="tower_pairs",
    )(own, *pieces, cotangent)


def tower_piece(own, pairs, cotangent, parts, k):
    tall, cols = pairs.shape
    quarter = cotangent.shape[0] // parts
    step = 512

    def body(own_ref, pairs_ref, cot_ref, out_ref, acc):
        i = pl.program_id(0)

        @pl.when(i == 0)
        def _():
            acc[...] = jnp.zeros_like(acc)

        acc[...] += lax.dot_general(
            pairs_ref[...],
            cot_ref[...],
            (((1,), (1,)), ((), ())),
            preferred_element_type=jnp.float32,
        )

        @pl.when(i == pl.num_programs(0) - 1)
        def _():
            out_ref[...] = acc[...].astype(out_ref.dtype)

    return pl.pallas_call(
        body,
        out_shape=jax.ShapeDtypeStruct((tall, quarter), pairs.dtype),
        grid_spec=pltpu.PrefetchScalarGridSpec(
            num_scalar_prefetch=1,
            grid=(cols // step,),
            in_specs=[
                pl.BlockSpec((tall, step), lambda i, own_ref: (0, i)),
                pl.BlockSpec((quarter, step), lambda i, own_ref: (own_ref[0] ^ k, i)),
            ],
            out_specs=pl.BlockSpec((tall, quarter), lambda i, own_ref: (0, 0)),
            scratch_shapes=[pltpu.VMEM((tall, quarter), jnp.float32)],
        ),
        compiler_params=pltpu.CompilerParams(vmem_limit_bytes=16 * 1024 * 1024),
        cost_estimate=pl.CostEstimate(
            flops=2 * tall * quarter * cols, transcendentals=0, bytes_accessed=14_000_000
        ),
        name="tower_piece",
    )(own, pairs, cotangent)


def owner_step(parts, selected, squeezed, table, slot_index, w_ex, w_ext, w_sq, w_sqt, slots):
    tables, span, samples = parts.shape
    count, width, _ = selected.shape
    scale = 1.0 / width**0.5
    f32, bf16 = jnp.float32, jnp.bfloat16
    turn = 8
    bundle = 8

    def dot(a, b):
        return jnp.dot(a, b, preferred_element_type=f32)

    def body(table_ref, slot_ref, parts_ref, sel_ref, sq_ref, hd_ref, wex_ref, wext_ref, wsq_ref,
             wsqt_ref, out_ref, acc, ex, sp):
        step = pl.program_id(0)

        @pl.when(step == 0)
        def _():
            acc[...] = jnp.zeros_like(acc)

        for r in range(turn):
            for k in range(LIMIT):
                f = table_ref[(step * turn + r) * LIMIT + k]
                acc[f] += parts_ref[r, k * width : (k + 1) * width, :].astype(f32)

        @pl.when(step == pl.num_programs(0) - 1)
        def _():
            sq = sq_ref[...]
            pre = dot(wsq_ref[...], jnp.concatenate([sq, sq, sq], axis=0)) * scale
            gate = 1.0 / (1.0 + jnp.exp(-pre))
            ah, al = halves(pre * gate)
            ex[...] = dot(wex_ref[...], jnp.concatenate([ah, ah, al], axis=0))
            d_act = jnp.zeros(pre.shape, f32)
            for b in range(count // bundle):
                at = slice(b * bundle * width, (b + 1) * bundle * width)
                rows = sel_ref[b * bundle : (b + 1) * bundle].reshape(bundle * width, samples)
                fields = dot(hd_ref[...], rows) * scale
                got = acc[b * bundle : (b + 1) * bundle].reshape(bundle * width, samples)
                eh, el = halves(got * fields)
                d_act = d_act + dot(wext_ref[b, 0], eh) + dot(wext_ref[b, 0], el)
                d_act = d_act + dot(wext_ref[b, 1], eh)
                ex[at] = got * (1.0 + ex[at])
            d_pre = d_act * gate * (1.0 + pre * (1.0 - gate))
            ph, pl_ = halves(d_pre)
            sp[...] = dot(wsqt_ref[...], jnp.concatenate([ph, pl_, ph], axis=0)) * (1.0 / width)
            out_ref[...] = jnp.zeros_like(out_ref)
            for f in range(count):
                grad = ex[f * width : (f + 1) * width] + sp[f : f + 1, :]
                out_ref[slot_ref[f]] = grad.astype(bf16)

    hd = jnp.asarray(np.kron(np.eye(bundle), hadamard_np(width)), bf16)
    mats = (selected, squeezed, hd, w_ex, w_ext, w_sq, w_sqt)
    return pl.pallas_call(
        body,
        out_shape=jax.ShapeDtypeStruct((slots, width, samples), bf16),
        grid_spec=pltpu.PrefetchScalarGridSpec(
            num_scalar_prefetch=2,
            grid=(tables // turn,),
            in_specs=[
                pl.BlockSpec((turn, span, samples), lambda i, *_: (i, 0, 0)),
                *[pl.BlockSpec(m.shape, lambda i, *_, n=m.ndim: (0,) * n) for m in mats],
            ],
            out_specs=pl.BlockSpec((slots, width, samples), lambda i, *_: (0, 0, 0)),
            scratch_shapes=[
                pltpu.VMEM((count, width, samples), f32),
                pltpu.VMEM((count * width, samples), f32),
                pltpu.VMEM((count, samples), f32),
            ],
        ),
        compiler_params=pltpu.CompilerParams(vmem_limit_bytes=40 * 1024 * 1024),
        name="owner_step",
    )(table, slot_index, parts, *mats)


def pair_step(got, pair_grad, left, right, signs, w_pairs, w_ex, w_ext, w_sq, width):
    tables, tall, samples = got.shape
    slots = left.shape[0]
    units = w_sq.shape[0]
    count = tall - LIMIT * width
    span = LIMIT * width
    group = 4
    cols = group * samples
    scale = 1.0 / width**0.5
    f32, bf16 = jnp.float32, jnp.bfloat16

    def dot(a, b):
        return jnp.dot(a, b, preferred_element_type=f32)

    def dot_nt(a, b):
        return lax.dot_general(a, b, (((1,), (1,)), ((), ())), preferred_element_type=f32)

    half = (LIMIT + 1) // 2 * width
    spans = [slice(0, half), slice(half, span)]

    def blocks(a, b):
        return jnp.concatenate([dot(a[s, : s.stop - s.start], b[s]) for s in spans], axis=0)

    def body(left_ref, right_ref, got_ref, pg_ref, hd_ref, rep_ref, rept_ref, mask_ref, wb_ref,
             wex_ref, wext_ref, wsq_ref, pairs_ref, part_ref, dbil_ref, dex_ref, dsq_ref,
             wt, mp, dm, dw, mats):
        @pl.when(pl.program_id(0) == 0)
        def _():
            for k in range(4):
                tall = dot(rep_ref[...], wb_ref[k]).astype(bf16)
                mats[k] = (dot(tall, rept_ref[...]) * mask_ref[...]).astype(bf16)
            dbil_ref[...] = jnp.zeros_like(dbil_ref)
            dex_ref[...] = jnp.zeros_like(dex_ref)
            dsq_ref[...] = jnp.zeros_like(dsq_ref)

        rows = jnp.concatenate([got_ref[o] for o in range(group)], axis=1)
        sq = rows[span:]
        fields = blocks(hd_ref, rows[:span]) * scale
        pre = dot(wsq_ref[...], jnp.concatenate([sq, sq, sq], axis=0)) * scale
        gate = 1.0 / (1.0 + jnp.exp(-pre))
        act = pre * gate
        ah, al = halves(act)
        excite = dot(wex_ref[...], jnp.concatenate([ah, ah, al], axis=0))
        weighted = fields * (1.0 + excite)
        wh, wl = halves(weighted)
        mapped = blocks(mats.at[0], wh) + blocks(mats.at[0], wl) + blocks(mats.at[1], wh)
        wt[...] = weighted.reshape(LIMIT, width, cols)
        mp[...] = mapped.reshape(LIMIT, width, cols)
        dm[...] = jnp.zeros_like(dm)
        dw[...] = jnp.zeros_like(dw)

        def one(p, carry):
            i = left_ref[p]
            j = right_ref[p]
            off = pl.multiple_of(p * width, width)
            x = mp[i]
            y = wt[j]
            pairs_ref[pl.ds(off, width), :] = (x * y).astype(bf16)
            g = pg_ref[pl.ds(off, width), :].astype(f32)
            dm[i] += g * y
            dw[j] += g * x
            return carry

        lax.fori_loop(0, slots, one, 0, unroll=2)
        dmv = dm[...].reshape(span, cols)
        dh, dl = halves(dmv)
        part = dw[...].reshape(span, cols) + (
            blocks(mats.at[2], dh) + blocks(mats.at[2], dl) + blocks(mats.at[3], dh)
        )
        sent = part.astype(bf16)
        for o in range(group):
            part_ref[o] = sent[:, o * samples : (o + 1) * samples]
        d_excite = part * fields
        eh, el = halves(d_excite)
        d_act = dot(wext_ref[...], jnp.concatenate([eh, el, eh], axis=0))
        d_pre = d_act * gate * (1.0 + pre * (1.0 - gate))
        ph, pl_ = halves(d_pre)

        for s in spans:
            dbil_ref[s, : s.stop - s.start] += dot_nt(wh[s], dh[s])
        dex_ref[...] += dot_nt(jnp.concatenate([ah, al], axis=0), eh)
        dsq_ref[...] += dot_nt(jnp.concatenate([ph, pl_], axis=0), sq)

    def whole(a):
        return pl.BlockSpec(a.shape, lambda i, *_, n=a.ndim: (0,) * n)

    block = np.kron(np.eye(LIMIT), np.ones((width, width)))
    turned = np.zeros((span, half), np.float32)
    mask = np.zeros((span, half), np.float32)
    for s in spans:
        turned[s, : s.stop - s.start] = np.kron(np.eye(LIMIT), signs)[s, s]
        mask[s, : s.stop - s.start] = block[s, s]
    repeat = np.tile(np.eye(width), (LIMIT, 1))
    mats = (
        jnp.asarray(turned, bf16),
        jnp.asarray(repeat, bf16),
        jnp.asarray(repeat[:half].T, bf16),
        jnp.asarray(mask, f32),
        w_pairs,
        w_ex,
        w_ext,
        w_sq,
    )
    return pl.pallas_call(
        body,
        out_shape=(
            jax.ShapeDtypeStruct((slots * width, tables * samples), bf16),
            jax.ShapeDtypeStruct((tables, span, samples), bf16),
            jax.ShapeDtypeStruct((span, half), f32),
            jax.ShapeDtypeStruct((2 * units, span), f32),
            jax.ShapeDtypeStruct((2 * units, count), f32),
        ),
        grid_spec=pltpu.PrefetchScalarGridSpec(
            num_scalar_prefetch=2,
            grid=(tables // group,),
            in_specs=[
                pl.BlockSpec((group, got.shape[1], samples), lambda i, *_: (i, 0, 0)),
                pl.BlockSpec((slots * width, cols), lambda i, *_: (0, i)),
                *[whole(m) for m in mats],
            ],
            out_specs=[
                pl.BlockSpec((slots * width, cols), lambda i, *_: (0, i)),
                pl.BlockSpec((group, span, samples), lambda i, *_: (i, 0, 0)),
                pl.BlockSpec((span, half), lambda i, *_: (0, 0)),
                pl.BlockSpec((2 * units, span), lambda i, *_: (0, 0)),
                pl.BlockSpec((2 * units, count), lambda i, *_: (0, 0)),
            ],
            scratch_shapes=[
                *[pltpu.VMEM((LIMIT, width, cols), f32) for _ in range(4)],
                pltpu.VMEM((4, span, half), bf16),
            ],
        ),
        compiler_params=pltpu.CompilerParams(vmem_limit_bytes=40 * 1024 * 1024),
        name="pair_step",
    )(left, right, got, pair_grad, *mats)


def on_device(pooled, field_owner, w_squeeze, w_excite, w_bilinear, tower_weight, tower_cotangent):
    f32, bf16 = jnp.float32, jnp.bfloat16
    per_owner, _, _, width, samples = pooled.shape
    tables, subs = lax.axis_size("table"), lax.axis_size("sub")
    total_samples = tables * subs * samples
    count = field_owner.shape[0]
    rows, hidden = tower_weight.shape
    plan = make_plan(count, tables, subs, width, rows)
    plane, depth, unit, units = plan["plane"], plan["depth"], plan["unit"], plan["units"]
    quarter = hidden // subs
    scale = 1.0 / width**0.5
    signs_np = hadamard_np(width)
    signs = jnp.asarray(signs_np, bf16)
    here = lax.axis_index("table")

    rotated = (
        jnp.einsum("ij,ktsjb->ktsib", signs, pooled, preferred_element_type=f32) * scale
    ).astype(bf16)
    rotated, tower_weight = lax.optimization_barrier((rotated, tower_weight))
    received = lax.all_to_all(rotated, "table", split_axis=1, concat_axis=0, tiled=True)
    received = received.reshape(per_owner * tables, width, samples)

    cut = jnp.moveaxis(tower_weight.reshape(rows, subs, quarter), 1, 0)
    cut = xor_order(cut, "sub")
    cut = trade([cut[k] for k in range(subs)], "sub", subs)

    slot_index = slot_table(field_owner, per_owner)
    table = jnp.asarray(plan["table"].reshape(-1))
    selected = jnp.take(received, slot_index, axis=0, mode="clip")
    squeeze_rows = selected[:, 0, :]

    cut = xor_order(jnp.stack(cut), "sub").reshape(units, unit, quarter)
    cut = jnp.concatenate([cut, jnp.zeros((1, unit, quarter), bf16)], axis=0)
    cut = jnp.take(cut, jnp.asarray(plan["pick"])[here], axis=0, mode="clip")
    cut = cut.reshape(plane, depth * width, quarter)

    sent = pack_rows(received, squeeze_rows, slot_index, table)
    sent, cut = lax.optimization_barrier((sent, cut))
    got = lax.all_to_all(sent, "table", split_axis=0, concat_axis=0, tiled=True)
    cut = trade([cut[k] for k in range(plane)], "table", tables)
    cut = jnp.concatenate(cut, axis=0)
    pieces = trade([cut] * subs, "sub", subs)

    cotangent = lax.all_gather(tower_cotangent, "table", axis=1, tiled=True)
    own_sub = lax.axis_index("sub")
    pair_grad = tower_pairs(own_sub[None], pieces, cotangent)

    xh, xl = halves(w_excite)
    mine = jnp.asarray(plan["table"])[here]
    here_h, here_l = [
        jnp.take(x.reshape(count, width, -1), mine, axis=0, mode="clip").reshape(LIMIT * width, -1)
        for x in (xh, xl)
    ]
    s1, s2 = halves(w_squeeze)
    s3 = (w_squeeze - s1.astype(f32) - s2.astype(f32)).astype(bf16)
    w_sq = jnp.concatenate([s1, s2, s3], axis=1)
    pairs, part, d_bilinear, d_excite, d_squeeze = pair_step(
        got,
        pair_grad,
        jnp.asarray(plan["left"])[here],
        jnp.asarray(plan["right"])[here],
        signs_np,
        jnp.stack([*halves(w_bilinear.T), *halves(w_bilinear)]),
        jnp.concatenate([here_h, here_l, here_h], axis=1),
        jnp.concatenate([here_h, here_h, here_l], axis=0).T,
        w_sq,
        width,
    )
    parts = lax.all_to_all(part, "table", split_axis=0, concat_axis=0, tiled=True)

    own_now = own_sub[None]
    total = [None] * subs
    for k in sorted(range(subs), key=lambda k: (k == 0, k != 2, k)):
        piece = tower_piece(own_now, pairs, cotangent, subs, k)
        own_now, piece = lax.optimization_barrier((own_now, piece))
        total[k] = swap(piece, "sub", subs, k) if k else piece
    d_excite, d_squeeze, d_bilinear, _ = lax.optimization_barrier(
        (d_excite, d_squeeze, d_bilinear, own_now)
    )
    total = sum(x.astype(f32) for x in total) * (1.0 / total_samples)
    bundled = [x.T.reshape(w_squeeze.shape[0], count // 8, 8 * width).transpose(1, 0, 2) for x in (xh, xl)]
    placed = owner_step(
        parts,
        selected,
        squeeze_rows,
        table,
        slot_index,
        jnp.concatenate([xh, xl, xh], axis=1),
        jnp.stack(bundled, axis=1),
        w_sq,
        jnp.concatenate([s1, s1, s2], axis=0).T,
        per_owner * tables,
    )
    total = total.astype(bf16)
    placed, total = lax.optimization_barrier((placed, total))
    placed = placed.reshape(per_owner * tables, 1, 1, width, samples)
    row_grads = lax.all_to_all(placed, "table", split_axis=0, concat_axis=1, tiled=True)
    total = total.reshape(plane, depth * width, quarter)
    total = trade([total[k] for k in range(plane)], "table", tables)
    total = jnp.concatenate(total, axis=0).reshape(-1, unit, quarter)
    total = jnp.take(total, jnp.asarray(plan["back"])[here], axis=0, mode="clip")
    total = xor_order(total.reshape(subs, rows, quarter), "sub")
    total = trade([total[k] for k in range(subs)], "sub", subs)
    total = xor_order(jnp.stack(total), "sub")
    weight_grad = jnp.moveaxis(total, 0, 1).reshape(rows, hidden).astype(f32)

    hidden_units = w_squeeze.shape[0]
    half = d_bilinear.shape[1]
    d_bilinear = sum(
        d_bilinear[k : k + width, k % half : k % half + width]
        for k in range(0, LIMIT * width, width)
    )
    d_excite = d_excite[:hidden_units] + d_excite[hidden_units:]
    d_squeeze = (d_squeeze[:hidden_units] + d_squeeze[hidden_units:]) * scale
    lift = (jnp.arange(count, dtype=jnp.int32)[:, None] == mine[None, :]) & jnp.asarray(
        plan["live"]
    )[here][None, :]
    d_excite = d_excite.reshape(hidden_units, LIMIT, width).transpose(1, 2, 0)
    d_excite = jnp.dot(
        lift.astype(f32), d_excite.reshape(LIMIT, width * hidden_units), precision=HIGH
    )
    small = jnp.concatenate([d_excite.reshape(-1), d_squeeze.reshape(-1), d_bilinear.reshape(-1)])
    ends = np.cumsum([w_excite.size, w_squeeze.size, w_bilinear.size])
    small = jnp.pad(small, (0, -small.size % 1024)).reshape(-1, 128)
    for axis, size in (("table", tables), ("sub", subs)):
        bit = 1
        while bit < size:
            small = small + swap(small, axis, size, bit)
            bit *= 2
    small = small.reshape(-1) * (1.0 / total_samples)
    g_excite = small[: ends[0]].reshape(w_excite.shape)
    g_squeeze = small[ends[0] : ends[1]].reshape(w_squeeze.shape)
    g_bilinear = small[ends[1] : ends[2]].reshape(w_bilinear.shape)

    return (row_grads, weight_grad, g_squeeze, g_excite, g_bilinear)


def solution(mesh):
    return jax.shard_map(
        on_device,
        mesh=mesh,
        in_specs=(
            P("table", None, "sub", None, None),
            P(),
            P(),
            P(),
            P(),
            P(BOTH, None),
            P(None, BOTH),
        ),
        out_specs=(P("table", None, "sub", None, None), P(BOTH, None), P(), P(), P()),
        check_vma=False,
    )
```

```python
import functools

import jax
import jax.numpy as jnp
import numpy as np
from jax import lax
from jax.experimental import pallas as pl
from jax.experimental.pallas import tpu as pltpu
from jax.sharding import PartitionSpec as P


HIGH = lax.Precision.HIGHEST
BOTH = ("table", "sub")
PLANES = 4
LIMIT = 13

WORKER = (
    4, 3, 2, 5, 0, 2, 4, 3, 7, 3, 0, 4, 6, 2, 2, 6, 6, 3, 4, 0, 3, 7, 1, 1, 5, 7, 6, 0, 5, 6, 7, 1, 2, 1, 5, 5, 1, 4, 3, 2, 2, 4, 7, 7, 0, 1, 5,
    5, 0, 6, 1, 6, 4, 3, 7, 3, 0, 4, 6, 2, 2, 1, 6, 3, 4, 0, 3, 0, 2, 1, 6, 7, 6, 0, 5, 6, 7, 1, 2, 1, 5, 5, 1, 4, 3, 2, 2, 4, 7, 7, 0, 1, 5, 1,
    5, 4, 3, 4, 3, 7, 3, 0, 4, 6, 2, 2, 6, 6, 3, 4, 0, 3, 7, 2, 1, 6, 7, 6, 0, 5, 6, 7, 1, 2, 1, 5, 5, 1, 4, 3, 2, 2, 4, 5, 7, 0, 1, 5, 7, 3, 4,
    4, 3, 7, 3, 0, 4, 6, 2, 2, 6, 6, 3, 4, 0, 3, 0, 1, 1, 5, 7, 6, 0, 5, 6, 7, 1, 2, 1, 5, 5, 1, 4, 3, 2, 2, 4, 5, 7, 0, 5, 5, 1, 7, 4, 3, 7, 3,
    0, 4, 6, 2, 2, 6, 6, 3, 4, 0, 3, 0, 2, 1, 5, 7, 6, 0, 5, 6, 7, 1, 2, 1, 5, 5, 1, 4, 3, 2, 2, 4, 5, 7, 0, 5, 5, 0, 4, 3, 7, 3, 0, 4, 6, 2, 2,
    6, 6, 3, 4, 0, 3, 7, 2, 1, 6, 7, 6, 0, 5, 6, 7, 1, 2, 1, 5, 5, 1, 4, 3, 2, 2, 4, 7, 7, 0, 5, 5, 4, 3, 7, 3, 0, 4, 6, 2, 2, 6, 6, 3, 4, 0, 3,
    1, 5, 7, 6, 6, 4, 0, 1, 5, 2, 1, 4, 7, 0, 6, 0, 6, 3, 4, 7, 1, 7, 3, 0, 3, 5, 6, 0, 2, 3, 2, 4, 3, 2, 4, 1, 5, 3, 2, 2, 1, 5, 7, 6, 6, 4, 0,
    1, 5, 2, 1, 4, 7, 0, 6, 0, 6, 3, 4, 7, 1, 7, 3, 0, 3, 5, 7, 4, 3, 6, 5, 3, 2, 4, 1, 5, 3, 2, 2, 1, 5, 7, 6, 6, 4, 2, 1, 5, 2, 1, 4, 7, 0, 6,
    0, 6, 3, 4, 7, 1, 7, 6, 0, 3, 5, 7, 0, 3, 5, 3, 2, 4, 1, 5, 3, 2, 2, 1, 5, 7, 0, 6, 4, 2, 1, 5, 2, 1, 4, 7, 0, 6, 0, 6, 3, 4, 7, 1, 7, 3, 0,
    3, 5, 3, 7, 5, 3, 2, 4, 1, 5, 3, 2, 2, 1, 5, 7, 0, 6, 4, 2, 1, 5, 2, 1, 4, 7, 0, 6, 0, 6, 3, 4, 7, 1, 7, 6, 0, 3, 5, 5, 4, 3, 2, 4, 1, 5, 3,
    2, 2, 1, 5, 7, 0, 6, 4, 0, 1, 5, 2, 1, 4, 7, 0, 6, 0, 6, 3, 4, 7, 1, 7, 3, 0, 3, 5, 2, 3, 2, 4, 1, 5, 3, 2, 2, 1, 5, 7, 0, 6, 4, 0, 1, 5, 2,
    1, 4, 7, 0, 6, 0, 6, 3, 4, 7, 1, 7, 6, 0, 3, 5, 3, 2, 4, 1, 5, 3, 2, 2, 1, 5, 7, 0, 6, 4, 2, 1, 5, 2, 1, 4, 7, 0, 6, 0, 6, 3, 4, 7, 1, 7, 6,
    7, 7, 7, 4, 1, 1, 5, 6, 0, 4, 4, 5, 6, 5, 6, 2, 6, 0, 2, 3, 0, 2, 1, 4, 0, 5, 2, 3, 3, 5, 3, 1, 1, 2, 6, 3, 1, 4, 7, 6, 1, 5, 5, 2, 0, 5, 6,
    2, 6, 6, 0, 4, 2, 2, 1, 4, 0, 5, 2, 0, 0, 5, 4, 1, 1, 7, 7, 7, 4, 7, 6, 5, 4, 4, 3, 0, 5, 7, 4, 6, 6, 0, 3, 0, 7, 1, 3, 0, 5, 4, 3, 0, 5, 3,
    1, 1, 7, 7, 7, 1, 5, 1, 6, 4, 2, 6, 5, 6, 4, 6, 6, 2, 3, 2, 2, 1, 4, 3, 5, 2, 3, 3, 5, 4, 1, 1, 2, 6, 3, 7, 4, 1, 1, 5, 0, 5, 7, 4, 7, 0, 0,
    4, 0, 7, 1, 4, 0, 5, 4, 0, 0, 5, 4, 1, 1, 7, 7, 7, 6, 5, 7, 1, 6, 5, 6, 2, 6, 6, 2, 3, 2, 2, 1, 3, 3, 5, 2, 3, 3, 5, 3, 1, 1, 7, 6, 3, 2, 7,
    5, 6, 5, 6, 4, 7, 0, 2, 4, 0, 2, 1, 4, 0, 5, 4, 0, 0, 5, 4, 1, 1, 7, 7, 7, 1, 2, 6, 5, 6, 4, 6, 6, 2, 4, 2, 2, 1, 4, 3, 5, 4, 3, 3, 5, 3, 1,
    1, 2, 6, 3, 1, 0, 5, 7, 4, 7, 0, 0, 4, 0, 7, 1, 4, 0, 5, 4, 0, 0, 5, 4, 1, 1, 7, 7, 7, 6, 5, 6, 2, 6, 6, 2, 3, 2, 2, 1, 3, 3, 5, 2, 3, 3, 5,
    6, 6, 6, 1, 1, 1, 3, 5, 7, 5, 7, 0, 7, 0, 5, 0, 2, 3, 0, 5, 2, 0, 2, 5, 7, 3, 2, 7, 3, 3, 4, 2, 4, 1, 1, 4, 1, 3, 2, 3, 4, 2, 2, 4, 2, 4, 4,
    3, 2, 1, 1, 0, 6, 7, 5, 0, 0, 7, 3, 6, 6, 7, 5, 0, 5, 6, 7, 5, 6, 3, 7, 3, 6, 4, 6, 7, 3, 7, 0, 6, 7, 4, 3, 3, 0, 0, 4, 6, 4, 4, 7, 3, 1, 1,
    5, 2, 1, 2, 6, 1, 5, 2, 2, 1, 2, 5, 5, 6, 2, 6, 5, 1, 7, 4, 1, 4, 2, 7, 4, 2, 7, 1, 2, 4, 2, 7, 4, 7, 1, 5, 3, 0, 3, 6, 3, 0, 3, 0, 1, 6, 5,
    6, 6, 1, 6, 6, 5, 7, 4, 4, 1, 7, 5, 0, 1, 0, 7, 5, 7, 4, 7, 1, 5, 0, 2, 3, 5, 2, 3, 4, 0, 4, 2, 0, 3, 2, 3, 0, 1, 7, 5, 5, 7, 5, 0, 5, 5, 7,
    1, 1, 1, 2, 3, 4, 3, 0, 4, 0, 4, 4, 0, 3, 2, 3, 6, 4, 2, 2, 1, 6, 6, 6, 4, 2, 1, 1, 7, 3, 3, 1, 6, 6, 6, 3, 1, 6, 1, 5, 7, 0, 0, 4, 4, 4, 4,
    7, 5, 3, 5, 2, 5, 2, 3, 2, 2, 5, 0, 0, 7, 2, 3, 2, 2, 3, 0, 4, 5, 0, 1, 1, 5, 6, 6, 0, 2, 2, 6, 5, 6, 4, 7, 5, 7, 4, 7, 5, 3, 7, 3, 1, 1, 6,
)


@functools.lru_cache(maxsize=None)
def make_plan(count, tables, subs, width, rows):
    plane = tables // PLANES
    held = rows * subs
    unit = 8
    assert width % unit == 0 and held % unit == 0
    pairs = [(i, j) for i in range(count) for j in range(i + 1, count)]
    assert len(pairs) == len(WORKER) and len(pairs) * width == held * tables
    per_plane = len(pairs) // PLANES
    worker = [plane * (g // per_plane) + WORKER[g] for g in range(len(pairs))]
    fields = [set() for _ in range(tables)]
    for g, r in enumerate(worker):
        fields[r] |= set(pairs[g])
    fields = [sorted(s) for s in fields]
    assert max(len(s) for s in fields) <= LIMIT
    table = np.zeros((tables, LIMIT), np.int32)
    live = np.zeros((tables, LIMIT), bool)
    for r, s in enumerate(fields):
        table[r, : len(s)] = s
        live[r, : len(s)] = True
    touched = [[[] for _ in range(plane)] for _ in range(tables)]
    for t in range(tables):
        for g in range(held * t // width, (held * (t + 1) - 1) // width + 1):
            assert worker[g] // plane == t // plane
            touched[t][worker[g] % plane].append(g)
    depth = max(len(x) for y in touched for x in y)
    units = held // unit
    per = width // unit
    pick = np.full((tables, plane, depth, per), units, np.int32)
    back = np.zeros((tables, units), np.int32)
    left = np.zeros((tables, plane * depth), np.int32)
    right = np.zeros((tables, plane * depth), np.int32)
    for t in range(tables):
        for w in range(plane):
            for c, g in enumerate(touched[t][w]):
                r = t // plane * plane + w
                k = (t % plane) ^ w
                slot = k * depth + c
                left[r, slot] = fields[r].index(pairs[g][0])
                right[r, slot] = fields[r].index(pairs[g][1])
                for q in range(per):
                    u = (width * g - held * t) // unit + q
                    if 0 <= u < units:
                        pick[t, k, c, q] = u
                        back[t, u] = (k * depth + c) * per + q
    return dict(
        table=table, live=live, depth=depth, pick=pick.reshape(tables, -1), back=back,
        left=left, right=right, plane=plane, unit=unit, units=units,
    )


def hadamard_np(width):
    index = np.arange(width)
    both = index[:, None] & index[None, :]
    parity = np.zeros((width, width), int)
    for bit_pos in range(width.bit_length()):
        parity = parity ^ (both >> bit_pos & 1)
    return (1 - 2 * parity).astype(np.float32)


def slot_table(field_owner, per_owner):
    count = field_owner.shape[0]
    order = jnp.arange(count, dtype=jnp.int32)
    same = field_owner[:, None] == field_owner[None, :]
    earlier = order[:, None] > order[None, :]
    position = jnp.sum((same & earlier).astype(jnp.int32), axis=1)
    return field_owner * per_owner + position


def swap(value, axis, size, k):
    return lax.ppermute(value, axis, [(a, a ^ k) for a in range(size)])


def trade(blocks, axis, size):
    return [blocks[0]] + [swap(b, axis, size, k) for k, b in enumerate(blocks) if k]


def sum_of_four(value, axis, size, step):
    one, two, three = [swap(value, axis, size, k * step) for k in (1, 2, 3)]
    return (value + one) + (two + three)


def xor_order(blocks, axis):
    own = lax.axis_index(axis)
    return jnp.take(blocks, own ^ jnp.arange(blocks.shape[0], dtype=jnp.int32), axis=0, mode="clip")


def off_chip(x):
    return pltpu.with_memory_space_constraint(x, pltpu.HBM)


def halves(x):
    high = x.astype(jnp.bfloat16)
    return high, (x - high.astype(jnp.float32)).astype(jnp.bfloat16)


def pack_rows(received, squeezed, slot_index, table):
    slots, width, samples = received.shape
    count = squeezed.shape[0]
    tables = table.shape[0] // LIMIT
    total = LIMIT * width + count
    turn = 8

    def body(slot_ref, table_ref, received_ref, squeezed_ref, out_ref):
        first = pl.program_id(0) * (turn * LIMIT)
        for r in range(turn):
            for k in range(LIMIT):
                out_ref[r, k * width : (k + 1) * width, :] = received_ref[
                    slot_ref[table_ref[first + r * LIMIT + k]]
                ]
            out_ref[r, LIMIT * width :, :] = squeezed_ref[...]

    return pl.pallas_call(
        body,
        out_shape=jax.ShapeDtypeStruct((tables, total, samples), received.dtype),
        grid_spec=pltpu.PrefetchScalarGridSpec(
            num_scalar_prefetch=2,
            grid=(tables // turn,),
            in_specs=[
                pl.BlockSpec((slots, width, samples), lambda i, *_: (0, 0, 0)),
                pl.BlockSpec((count, samples), lambda i, *_: (0, 0)),
            ],
            out_specs=pl.BlockSpec((turn, total, samples), lambda i, *_: (i, 0, 0)),
        ),
        name="pack_rows",
    )(slot_index, table, received, squeezed)


def tower_pairs(own, pieces, cotangent):
    tall, quarter = pieces[0].shape
    hidden, cols = cotangent.shape
    parts = len(pieces)
    step = 512

    def body(own_ref, *refs):
        cot_ref, out_ref, rows_ref = refs[parts:]

        @pl.when(pl.program_id(0) == 0)
        def _():
            for o in range(parts):

                @pl.when(own_ref[0] == o)
                def _(o=o):
                    for q in range(parts):
                        rows_ref[:, q * quarter : (q + 1) * quarter] = refs[o ^ q][...]

        out_ref[...] = jnp.dot(
            rows_ref[...], cot_ref[...], preferred_element_type=jnp.float32
        ).astype(out_ref.dtype)

    return pl.pallas_call(
        body,
        out_shape=jax.ShapeDtypeStruct((tall, cols), cotangent.dtype),
        grid_spec=pltpu.PrefetchScalarGridSpec(
            num_scalar_prefetch=1,
            grid=(cols // step,),
            in_specs=[
                *[pl.BlockSpec((tall, quarter), lambda i, *_: (0, 0)) for _ in pieces],
                pl.BlockSpec((hidden, step), lambda i, *_: (0, i)),
            ],
            out_specs=pl.BlockSpec((tall, step), lambda i, *_: (0, i)),
            scratch_shapes=[pltpu.VMEM((tall, hidden), cotangent.dtype)],
        ),
        compiler_params=pltpu.CompilerParams(vmem_limit_bytes=40 * 1024 * 1024),
        cost_estimate=pl.CostEstimate(
            flops=2 * tall * hidden * cols, transcendentals=0, bytes_accessed=30_000_000
        ),
        name="tower_pairs",
    )(own, *[off_chip(p) for p in pieces], off_chip(cotangent))


def tower_total(own, pairs, cotangent, parts):
    tall, cols = pairs.shape
    hidden = cotangent.shape[0]
    quarter = hidden // parts
    step = 512

    def body(own_ref, pairs_ref, cot_ref, *refs):
        outs, acc = refs[:parts], refs[parts]
        i = pl.program_id(0)

        @pl.when(i == 0)
        def _():
            acc[...] = jnp.zeros_like(acc)

        acc[...] += lax.dot_general(
            pairs_ref[...],
            cot_ref[...],
            (((1,), (1,)), ((), ())),
            preferred_element_type=jnp.float32,
        )

        @pl.when(i == pl.num_programs(0) - 1)
        def _():
            for o in range(parts):

                @pl.when(own_ref[0] == o)
                def _(o=o):
                    for k in range(parts):
                        q = o ^ k
                        outs[k][...] = acc[:, q * quarter : (q + 1) * quarter].astype(
                            pairs.dtype
                        )

    return pl.pallas_call(
        body,
        out_shape=[jax.ShapeDtypeStruct((tall, quarter), pairs.dtype)] * parts,
        grid_spec=pltpu.PrefetchScalarGridSpec(
            num_scalar_prefetch=1,
            grid=(cols // step,),
            in_specs=[
                pl.BlockSpec((tall, step), lambda i, *_: (0, i)),
                pl.BlockSpec((hidden, step), lambda i, *_: (0, i)),
            ],
            out_specs=[pl.BlockSpec((tall, quarter), lambda i, *_: (0, 0))] * parts,
            scratch_shapes=[pltpu.VMEM((tall, hidden), jnp.float32)],
        ),
        compiler_params=pltpu.CompilerParams(vmem_limit_bytes=32 * 1024 * 1024),
        cost_estimate=pl.CostEstimate(
            flops=2 * tall * hidden * cols, transcendentals=0, bytes_accessed=20_000_000
        ),
        name="tower_total",
    )(own, off_chip(pairs), off_chip(cotangent))


def owner_step(parts, selected, squeezed, table, slot_index, w_ex, w_ext, w_sq, w_sqt, slots):
    tables, span, samples = parts.shape
    count, width, _ = selected.shape
    scale = 1.0 / width**0.5
    f32, bf16 = jnp.float32, jnp.bfloat16
    turn = 8
    bundle = 8

    def dot(a, b):
        return jnp.dot(a, b, preferred_element_type=f32)

    def body(table_ref, slot_ref, parts_ref, sel_ref, sq_ref, hd_ref, wex_ref, wext_ref, wsq_ref,
             wsqt_ref, out_ref, acc, ex, sp):
        step = pl.program_id(0)

        @pl.when(step == 0)
        def _():
            acc[...] = jnp.zeros_like(acc)

        for r in range(turn):
            for k in range(LIMIT):
                f = table_ref[(step * turn + r) * LIMIT + k]
                acc[f] += parts_ref[r, k * width : (k + 1) * width, :].astype(f32)

        @pl.when(step == pl.num_programs(0) - 1)
        def _():
            sq = sq_ref[...]
            pre = dot(wsq_ref[...], jnp.concatenate([sq, sq, sq], axis=0)) * scale
            gate = 1.0 / (1.0 + jnp.exp(-pre))
            ah, al = halves(pre * gate)
            ex[...] = dot(wex_ref[...], jnp.concatenate([ah, ah, al], axis=0))
            d_act = jnp.zeros(pre.shape, f32)
            for b in range(count // bundle):
                at = slice(b * bundle * width, (b + 1) * bundle * width)
                rows = sel_ref[b * bundle : (b + 1) * bundle].reshape(bundle * width, samples)
                fields = dot(hd_ref[...], rows) * scale
                got = acc[b * bundle : (b + 1) * bundle].reshape(bundle * width, samples)
                eh, el = halves(got * fields)
                d_act = d_act + dot(wext_ref[b, 0], eh) + dot(wext_ref[b, 0], el)
                d_act = d_act + dot(wext_ref[b, 1], eh)
                ex[at] = got * (1.0 + ex[at])
            d_pre = d_act * gate * (1.0 + pre * (1.0 - gate))
            ph, pl_ = halves(d_pre)
            sp[...] = dot(wsqt_ref[...], jnp.concatenate([ph, pl_, ph], axis=0)) * (1.0 / width)
            out_ref[...] = jnp.zeros_like(out_ref)
            for f in range(count):
                grad = ex[f * width : (f + 1) * width] + sp[f : f + 1, :]
                out_ref[slot_ref[f]] = grad.astype(bf16)

    hd = jnp.asarray(np.kron(np.eye(bundle), hadamard_np(width)), bf16)
    mats = (selected, squeezed, hd, w_ex, w_ext, w_sq, w_sqt)
    return pl.pallas_call(
        body,
        out_shape=jax.ShapeDtypeStruct((slots, width, samples), bf16),
        grid_spec=pltpu.PrefetchScalarGridSpec(
            num_scalar_prefetch=2,
            grid=(tables // turn,),
            in_specs=[
                pl.BlockSpec((turn, span, samples), lambda i, *_: (i, 0, 0)),
                *[pl.BlockSpec(m.shape, lambda i, *_, n=m.ndim: (0,) * n) for m in mats],
            ],
            out_specs=pl.BlockSpec((slots, width, samples), lambda i, *_: (0, 0, 0)),
            scratch_shapes=[
                pltpu.VMEM((count, width, samples), f32),
                pltpu.VMEM((count * width, samples), f32),
                pltpu.VMEM((count, samples), f32),
            ],
        ),
        compiler_params=pltpu.CompilerParams(vmem_limit_bytes=40 * 1024 * 1024),
        name="owner_step",
    )(table, slot_index, off_chip(parts), *mats)


def pair_step(got, pair_grad, left, right, signs, w_pairs, w_ex, w_ext, w_sq, width):
    tables, tall, samples = got.shape
    slots = left.shape[0]
    units = w_sq.shape[0]
    count = tall - LIMIT * width
    span = LIMIT * width
    group = 4
    cols = group * samples
    scale = 1.0 / width**0.5
    f32, bf16 = jnp.float32, jnp.bfloat16

    def dot(a, b):
        return jnp.dot(a, b, preferred_element_type=f32)

    def dot_nt(a, b):
        return lax.dot_general(a, b, (((1,), (1,)), ((), ())), preferred_element_type=f32)

    half = (LIMIT + 1) // 2 * width
    spans = [slice(0, half), slice(half, span)]

    def blocks(a, b):
        return jnp.concatenate([dot(a[s, : s.stop - s.start], b[s]) for s in spans], axis=0)

    def body(left_ref, right_ref, got_ref, pg_ref, hd_ref, rep_ref, rept_ref, mask_ref, wb_ref,
             wex_ref, wext_ref, wsq_ref, pairs_ref, part_ref, dbil_ref, dex_ref, dsq_ref,
             wt, mp, dm, dw, mats):
        @pl.when(pl.program_id(0) == 0)
        def _():
            for k in range(4):
                tall = dot(rep_ref[...], wb_ref[k]).astype(bf16)
                mats[k] = (dot(tall, rept_ref[...]) * mask_ref[...]).astype(bf16)
            dbil_ref[...] = jnp.zeros_like(dbil_ref)
            dex_ref[...] = jnp.zeros_like(dex_ref)
            dsq_ref[...] = jnp.zeros_like(dsq_ref)

        rows = jnp.concatenate([got_ref[o] for o in range(group)], axis=1)
        sq = rows[span:]
        fields = blocks(hd_ref, rows[:span]) * scale
        pre = dot(wsq_ref[...], jnp.concatenate([sq, sq, sq], axis=0)) * scale
        gate = 1.0 / (1.0 + jnp.exp(-pre))
        act = pre * gate
        ah, al = halves(act)
        excite = dot(wex_ref[...], jnp.concatenate([ah, ah, al], axis=0))
        weighted = fields * (1.0 + excite)
        wh, wl = halves(weighted)
        mapped = blocks(mats.at[0], wh) + blocks(mats.at[0], wl) + blocks(mats.at[1], wh)
        wt[...] = weighted.reshape(LIMIT, width, cols)
        mp[...] = mapped.reshape(LIMIT, width, cols)
        dm[...] = jnp.zeros_like(dm)
        dw[...] = jnp.zeros_like(dw)

        def one(p, carry):
            i = left_ref[p]
            j = right_ref[p]
            off = pl.multiple_of(p * width, width)
            x = mp[i]
            y = wt[j]
            pairs_ref[pl.ds(off, width), :] = (x * y).astype(bf16)
            g = pg_ref[pl.ds(off, width), :].astype(f32)
            dm[i] += g * y
            dw[j] += g * x
            return carry

        lax.fori_loop(0, slots, one, 0, unroll=2)
        dmv = dm[...].reshape(span, cols)
        dh, dl = halves(dmv)
        part = dw[...].reshape(span, cols) + (
            blocks(mats.at[2], dh) + blocks(mats.at[2], dl) + blocks(mats.at[3], dh)
        )
        sent = part.astype(bf16)
        for o in range(group):
            part_ref[o] = sent[:, o * samples : (o + 1) * samples]
        d_excite = part * fields
        eh, el = halves(d_excite)
        d_act = dot(wext_ref[...], jnp.concatenate([eh, el, eh], axis=0))
        d_pre = d_act * gate * (1.0 + pre * (1.0 - gate))
        ph, pl_ = halves(d_pre)

        for s in spans:
            dbil_ref[s, : s.stop - s.start] += dot_nt(wh[s], dh[s])
        dex_ref[...] += dot_nt(jnp.concatenate([ah, al], axis=0), eh)
        dsq_ref[...] += dot_nt(jnp.concatenate([ph, pl_], axis=0), sq)

    def whole(a):
        return pl.BlockSpec(a.shape, lambda i, *_, n=a.ndim: (0,) * n)

    block = np.kron(np.eye(LIMIT), np.ones((width, width)))
    turned = np.zeros((span, half), np.float32)
    mask = np.zeros((span, half), np.float32)
    for s in spans:
        turned[s, : s.stop - s.start] = np.kron(np.eye(LIMIT), signs)[s, s]
        mask[s, : s.stop - s.start] = block[s, s]
    repeat = np.tile(np.eye(width), (LIMIT, 1))
    mats = (
        jnp.asarray(turned, bf16),
        jnp.asarray(repeat, bf16),
        jnp.asarray(repeat[:half].T, bf16),
        jnp.asarray(mask, f32),
        w_pairs,
        w_ex,
        w_ext,
        w_sq,
    )
    return pl.pallas_call(
        body,
        out_shape=(
            jax.ShapeDtypeStruct((slots * width, tables * samples), bf16),
            jax.ShapeDtypeStruct((tables, span, samples), bf16),
            jax.ShapeDtypeStruct((span, half), f32),
            jax.ShapeDtypeStruct((2 * units, span), f32),
            jax.ShapeDtypeStruct((2 * units, count), f32),
        ),
        grid_spec=pltpu.PrefetchScalarGridSpec(
            num_scalar_prefetch=2,
            grid=(tables // group,),
            in_specs=[
                pl.BlockSpec((group, got.shape[1], samples), lambda i, *_: (i, 0, 0)),
                pl.BlockSpec((slots * width, cols), lambda i, *_: (0, i)),
                *[whole(m) for m in mats],
            ],
            out_specs=[
                pl.BlockSpec((slots * width, cols), lambda i, *_: (0, i)),
                pl.BlockSpec((group, span, samples), lambda i, *_: (i, 0, 0)),
                pl.BlockSpec((span, half), lambda i, *_: (0, 0)),
                pl.BlockSpec((2 * units, span), lambda i, *_: (0, 0)),
                pl.BlockSpec((2 * units, count), lambda i, *_: (0, 0)),
            ],
            scratch_shapes=[
                *[pltpu.VMEM((LIMIT, width, cols), f32) for _ in range(4)],
                pltpu.VMEM((4, span, half), bf16),
            ],
        ),
        compiler_params=pltpu.CompilerParams(vmem_limit_bytes=40 * 1024 * 1024),
        name="pair_step",
    )(left, right, off_chip(got), pair_grad, *mats)


def on_device(pooled, field_owner, w_squeeze, w_excite, w_bilinear, tower_weight, tower_cotangent):
    f32, bf16 = jnp.float32, jnp.bfloat16
    per_owner, _, _, width, samples = pooled.shape
    tables, subs = lax.axis_size("table"), lax.axis_size("sub")
    total_samples = tables * subs * samples
    count = field_owner.shape[0]
    rows, hidden = tower_weight.shape
    plan = make_plan(count, tables, subs, width, rows)
    plane, depth, unit, units = plan["plane"], plan["depth"], plan["unit"], plan["units"]
    quarter = hidden // subs
    scale = 1.0 / width**0.5
    signs_np = hadamard_np(width)
    signs = jnp.asarray(signs_np, bf16)
    here = lax.axis_index("table")

    rotated = (
        jnp.einsum("ij,ktsjb->ktsib", signs, pooled, preferred_element_type=f32) * scale
    ).astype(bf16)
    rotated, tower_weight = lax.optimization_barrier((rotated, tower_weight))
    received = lax.all_to_all(rotated, "table", split_axis=1, concat_axis=0, tiled=True)
    received = received.reshape(per_owner * tables, width, samples)

    cut = jnp.moveaxis(tower_weight.reshape(rows, subs, quarter), 1, 0)
    cut = xor_order(cut, "sub")
    cut = trade([cut[k] for k in range(subs)], "sub", subs)

    slot_index = slot_table(field_owner, per_owner)
    table = jnp.asarray(plan["table"].reshape(-1))
    selected = jnp.take(received, slot_index, axis=0, mode="clip")
    squeeze_rows = selected[:, 0, :]

    cut = xor_order(jnp.stack(cut), "sub").reshape(units, unit, quarter)
    cut = jnp.concatenate([cut, jnp.zeros((1, unit, quarter), bf16)], axis=0)
    cut = jnp.take(cut, jnp.asarray(plan["pick"])[here], axis=0, mode="clip")
    cut = cut.reshape(plane, depth * width, quarter)

    sent = pack_rows(received, squeeze_rows, slot_index, table)
    got = lax.all_to_all(sent, "table", split_axis=0, concat_axis=0, tiled=True)
    cut = trade([cut[k] for k in range(plane)], "table", tables)
    cut = jnp.concatenate(cut, axis=0)
    pieces = trade([cut] * subs, "sub", subs)

    cotangent = lax.all_gather(tower_cotangent, "table", axis=1, tiled=True)
    own_sub = lax.axis_index("sub")
    pair_grad = tower_pairs(own_sub[None], pieces, cotangent)

    xh, xl = halves(w_excite)
    mine = jnp.asarray(plan["table"])[here]
    here_h, here_l = [
        jnp.take(x.reshape(count, width, -1), mine, axis=0, mode="clip").reshape(LIMIT * width, -1)
        for x in (xh, xl)
    ]
    s1, s2 = halves(w_squeeze)
    s3 = (w_squeeze - s1.astype(f32) - s2.astype(f32)).astype(bf16)
    w_sq = jnp.concatenate([s1, s2, s3], axis=1)
    pairs, part, d_bilinear, d_excite, d_squeeze = pair_step(
        got,
        pair_grad,
        jnp.asarray(plan["left"])[here],
        jnp.asarray(plan["right"])[here],
        signs_np,
        jnp.stack([*halves(w_bilinear.T), *halves(w_bilinear)]),
        jnp.concatenate([here_h, here_l, here_h], axis=1),
        jnp.concatenate([here_h, here_h, here_l], axis=0).T,
        w_sq,
        width,
    )
    parts = lax.all_to_all(part, "table", split_axis=0, concat_axis=0, tiled=True)

    total = tower_total(own_sub[None], pairs, cotangent, subs)
    sent = [total[0]]
    for k in range(1, subs):
        sent.append(swap(total[k], "sub", subs, k))
    total = sent
    total = sum(x.astype(f32) for x in total) * (1.0 / total_samples)
    bundled = [x.T.reshape(w_squeeze.shape[0], count // 8, 8 * width).transpose(1, 0, 2) for x in (xh, xl)]
    placed = owner_step(
        parts,
        selected,
        squeeze_rows,
        table,
        slot_index,
        jnp.concatenate([xh, xl, xh], axis=1),
        jnp.stack(bundled, axis=1),
        w_sq,
        jnp.concatenate([s1, s1, s2], axis=0).T,
        per_owner * tables,
    )
    total = total.astype(bf16)
    placed = placed.reshape(per_owner * tables, 1, 1, width, samples)
    row_grads = lax.all_to_all(placed, "table", split_axis=0, concat_axis=1, tiled=True)
    total = total.reshape(plane, depth * width, quarter)
    total = trade([total[k] for k in range(plane)], "table", tables)
    total = jnp.concatenate(total, axis=0).reshape(-1, unit, quarter)
    total = jnp.take(total, jnp.asarray(plan["back"])[here], axis=0, mode="clip")
    total = xor_order(total.reshape(subs, rows, quarter), "sub")
    total = trade([total[k] for k in range(subs)], "sub", subs)
    total = xor_order(jnp.stack(total), "sub")
    weight_grad = jnp.moveaxis(total, 0, 1).reshape(rows, hidden).astype(f32)

    hidden_units = w_squeeze.shape[0]
    half = d_bilinear.shape[1]
    d_bilinear = sum(
        d_bilinear[k : k + width, k % half : k % half + width]
        for k in range(0, LIMIT * width, width)
    )
    d_excite = d_excite[:hidden_units] + d_excite[hidden_units:]
    d_squeeze = (d_squeeze[:hidden_units] + d_squeeze[hidden_units:]) * scale
    lift = (jnp.arange(count, dtype=jnp.int32)[:, None] == mine[None, :]) & jnp.asarray(
        plan["live"]
    )[here][None, :]
    d_excite = d_excite.reshape(hidden_units, LIMIT, width).transpose(1, 2, 0)
    d_excite = jnp.dot(
        lift.astype(f32), d_excite.reshape(LIMIT, width * hidden_units), precision=HIGH
    )
    small = jnp.concatenate([d_excite.reshape(-1), d_squeeze.reshape(-1), d_bilinear.reshape(-1)])
    ends = np.cumsum([w_excite.size, w_squeeze.size, w_bilinear.size])
    small = jnp.pad(small, (0, -small.size % 1024)).reshape(-1, 128)
    small = small + swap(small, "table", tables, 1)
    small = sum_of_four(small, "sub", subs, 1)
    for bit in range(1, tables.bit_length() - 1, 2):
        small = sum_of_four(small, "table", tables, 2**bit)
    small = small.reshape(-1) * (1.0 / total_samples)
    g_excite = small[: ends[0]].reshape(w_excite.shape)
    g_squeeze = small[ends[0] : ends[1]].reshape(w_squeeze.shape)
    g_bilinear = small[ends[1] : ends[2]].reshape(w_bilinear.shape)

    return (row_grads, weight_grad, g_squeeze, g_excite, g_bilinear)


def solution(mesh):
    return jax.shard_map(
        on_device,
        mesh=mesh,
        in_specs=(
            P("table", None, "sub", None, None),
            P(),
            P(),
            P(),
            P(),
            P(BOTH, None),
            P(None, BOTH),
        ),
        out_specs=(P("table", None, "sub", None, None), P(BOTH, None), P(), P(), P()),
        check_vma=False,
    )
```
